32 devices in a mesh: aa: 8 (over z, y), ba: 4 (over x, core).
Axes of the slice: x: 2, y: 2, z: 4, core: 2. Of those that a mesh axis runs over, the one named last changes fastest.
Arguments:
- features: bfloat16 [65536, 256], P(('aa', 'ba')), may hold values from -6 to 6
- tile_ids: int32 [65536, 1], P(('aa', 'ba')), may hold values from 0 to 31; in each aligned block of 2048 rows (0 to 2047, 2048 to 4095, ...) at most 96 rows name the same one
- cell_ids: int32 [65536], P(('aa', 'ba')), may hold values from 0 to 8191
- spread_weight: float32 [65536], P(('aa', 'ba')), may hold values from 0.1 to 0.6
- read_weight: float32 [65536], P(('aa', 'ba')), may hold values from 0.5 to 2
- message_weight: bfloat16 [256, 256], replicated, may hold values from -0.375 to 0.375
- skip_weight: bfloat16 [256, 256], replicated, may hold values from -0.375 to 0.375
- spectral_weight: bfloat16 [16, 256, 256, 256], P('ba', 'aa'), may hold values from -1.5 to 1.5
- hidden_weight: bfloat16 [256, 256], replicated, may hold values from -0.375 to 0.375
- output_weight: bfloat16 [256, 256], replicated, may hold values from -0.75 to 0.75
Outputs:
- point_out: bfloat16 [65536, 256], P(('aa', 'ba'))
The draws below stay inside these ranges and needn't reach their ends.
Inputs may be any that keep to these rules, and one draw needn't show every extreme that they name: `tile_ids`: among the rows of one device no index appears more than 96 times, and some index appears exactly 96 times.
All inputs are finite; a program needn't handle non-finite values.
Results may differ from the reference program's by a relative error of at most 0.015.
Values may be sent and summed in bfloat16 or wider, within the bound.
A program may use at most 64 MiB of HBM per device.

```python
import math
import jax
import jax.numpy as jnp
import numpy as np
from jax import lax

C = 256
G = 64
M = 16
P_DEV = 2048
POINTS = 65536
CAP = 96
GXD = 8
GYD = 16
CELLS_DEV = 8192
N_BA = 4
DEVICES = 32


def touch_ends(values, rng, low, largest):
    extent = values.shape
    index_at = [jax.random.randint(jax.random.fold_in(rng, axis), (), 0, extent[axis]) for axis in range(len(extent))]
    values = values.at[tuple(index_at)].set(low)
    longest = extent.index(max(extent))
    index_at[longest] = (index_at[longest] + 1) % extent[longest]
    return values.at[tuple(index_at)].set(largest)


def block_scale(stream_key, shape, pieces, low, top_value):
    factor_of, own = 1.0, jax.random.fold_in(stream_key, 6)
    for axis_at, shards_of in pieces:
        steps = jnp.exp(jax.random.uniform(jax.random.fold_in(own, axis_at), (shards_of,), jnp.float32, low / len(pieces), top_value / len(pieces)))
        factor_of = factor_of * jnp.repeat(steps, shape[axis_at] // shards_of).reshape([-1 if axis == axis_at else 1 for axis in range(len(shape))])
    return factor_of


def deal_out(own_key, own, number, rows, count, top, reach, lean):
    sequence = jax.random.permutation(own_key, count)
    heavy_load, usual = shares(count, rows * top, reach, lean, True), shares(count, rows * top, reach, lean, False)
    places = jnp.arange(count)

    def named(tallies, rotation):
        used = int((tallies > 0).sum())
        fixed = max(1, used // 4)
        moved = fixed + (places - fixed + rotation * (used - fixed)) % max(1, count - fixed)
        return jnp.zeros((count,), jnp.int32).at[sequence[jnp.where(places < fixed, places, moved)]].set(jnp.asarray(tallies, jnp.int32))

    tallies = jnp.where(number % 4 == 0, named(heavy_load, number // 4), named(usual, number - number // 4 - 1))
    mixed = jax.random.permutation(jax.random.fold_in(own, 3), count)
    giver, sink = mixed[0:count // 2 * 2:2], mixed[1:count // 2 * 2:2]
    margin = jnp.minimum(tallies[giver] - 1, reach - tallies[sink]) // 2
    margin = jnp.where((giver == sequence[0]) | (sink == sequence[0]) | (tallies[sink] == 0), 0, jnp.maximum(margin, 0))
    moved = jax.random.randint(jax.random.fold_in(own, 4), (count // 2,), 0, 1 << 20) % (margin + 1)
    tallies = tallies.at[giver].add(-moved).at[sink].add(moved)
    labels = jnp.searchsorted(jnp.cumsum(tallies), jnp.arange(rows * top), side="right").astype(jnp.int32)
    grid = labels.reshape(top, rows).T
    grid = grid[jax.random.permutation(jax.random.fold_in(own, 1), rows)]
    rotation = jax.random.randint(jax.random.fold_in(own, 2), (rows, 1), 0, top)
    return jnp.take_along_axis(grid, (jnp.arange(top)[None, :] + rotation) % top, axis=1)


def shares(count, total, bound, skew, full):
    loads = [(1 << 20) // math.isqrt(grade ** skew) + 1 for grade in range(1, count + 1)]
    largest = bound if full else min(bound, max(-(-total // count), total * loads[0] // sum(loads)))
    least = 1 if total - largest >= count - 1 else 0
    holding, spare = [largest] + [least] * (count - 1), total - largest - least * (count - 1)
    while spare > 0:
        candidates = [i for i in range(1, count) if holding[i] < largest] or [i for i in range(1, count) if holding[i] < bound]
        whole, budget = sum([loads[i] for i in candidates]), spare
        for i in candidates:
            more = min(bound - holding[i], max(1, budget * loads[i] // whole), spare)
            holding[i] = holding[i] + more
            spare = spare - more
    return np.array(holding)


def bell_draw(rng, shape, spread, most, shards=(), kind=jnp.bfloat16):
    entries = jax.random.normal(rng, shape, jnp.float32) * spread
    if len(shards) > 0:
        entries = block_scale(rng, shape, shards, -0.22, 0.18) * entries
    return jnp.clip(entries, min=-most, max=most).astype(kind)


def setup_inputs(seed: int = 0) -> dict:
    splits = jax.random.split(jax.random.key(seed), 11)
    features = bell_draw(splits[0], (POINTS, C), 1.0, 6.0, ((0, 32),))
    tile_ids_keys = jax.random.split(jax.random.fold_in(splits[1], 1), POINTS // P_DEV)
    tile_ids_turns = jax.random.permutation(jax.random.fold_in(splits[1], 3), POINTS // P_DEV)
    tile_ids = jax.vmap(lambda own, number: deal_out(jax.random.fold_in(splits[1], 2), own, number, P_DEV, DEVICES, 1, CAP, 2))(tile_ids_keys, tile_ids_turns).reshape((POINTS, 1))
    cell_ids = touch_ends(jax.random.randint(splits[2], (POINTS,), 0, CELLS_DEV), jax.random.fold_in(splits[2], 1), 0, CELLS_DEV - 1).astype(jnp.int32)
    spread_weight = jnp.clip(0.1 + 0.5 * jax.random.uniform(splits[3], (POINTS,), jnp.float32) ** block_scale(splits[3], (POINTS,), ((0, 32),), -0.2, 0.2), 0.1, 0.6)
    read_weight = jnp.clip(0.5 + 1.5 * jax.random.uniform(splits[4], (POINTS,), jnp.float32) ** block_scale(splits[4], (POINTS,), ((0, 32),), -0.2, 0.2), 0.5, 2.0)
    message_weight = bell_draw(splits[5], (C, C), C ** -0.5, 0.375)
    skip_weight = bell_draw(splits[6], (C, C), C ** -0.5, 0.375)
    spectral_weight = bell_draw(splits[7], (M, M * M, C, C), (C // 16) ** -0.5, 1.5, ((0, 4), (1, 8)))
    hidden_weight = bell_draw(splits[8], (C, C), C ** -0.5, 0.375)
    output_weight = bell_draw(splits[9], (C, C), (C // 4) ** -0.5, 0.75)
    return dict(features=features, tile_ids=tile_ids, cell_ids=cell_ids, spread_weight=spread_weight, read_weight=read_weight, message_weight=message_weight, skip_weight=skip_weight, spectral_weight=spectral_weight, hidden_weight=hidden_weight, output_weight=output_weight)


def basis_table(mode_count, grid_length, positions):
    mode_index = jnp.arange(mode_count, dtype=jnp.int32)[:, None]
    half_modes = mode_count // 2
    frequency = jnp.where(mode_index < half_modes, mode_index, mode_index - half_modes + 1).astype(jnp.float32)
    phase_angle = 2.0 * math.pi * frequency * positions.astype(jnp.float32)[None, :] / grid_length
    waveform = jnp.where(mode_index < half_modes, jnp.cos(phase_angle), jnp.sin(phase_angle))
    norm_scale = jnp.where(mode_index == 0, math.sqrt(1.0 / grid_length), math.sqrt(2.0 / grid_length))
    return (waveform * norm_scale).astype(jnp.float32)

def global_cell(tiles, cells):
    grid_x = tiles // N_BA * GXD + cells // (GYD * G)
    grid_y = tiles % N_BA * GYD + cells // G % GYD
    grid_z = cells % G
    return ((grid_x * G + grid_y) * G + grid_z).astype(jnp.int32)

def reference(features, tile_ids, cell_ids, spread_weight, read_weight, message_weight, skip_weight, spectral_weight, hidden_weight, output_weight):
    highest = lax.Precision.HIGHEST
    block_count = POINTS // P_DEV
    feat_blocks = features.reshape(block_count, P_DEV, C)
    tile_blocks = tile_ids.reshape(block_count, P_DEV)
    cell_blocks = cell_ids.reshape(block_count, P_DEV)
    spread_blocks = spread_weight.reshape(block_count, P_DEV)
    read_blocks = read_weight.reshape(block_count, P_DEV)

    def spread_step(latent_sum, block):
        feat_block, tile_block, cell_block, spread_block = block
        product = jnp.dot(feat_block, message_weight, preferred_element_type=jnp.float32)
        message = (spread_block[:, None] * product).astype(jnp.bfloat16)
        latent_sum = latent_sum.at[global_cell(tile_block, cell_block)].add(message.astype(jnp.float32))
        return (latent_sum, jnp.zeros((), jnp.float32))
    latent_sum, unused = lax.scan(spread_step, jnp.zeros((G * G * G, C), jnp.float32), (feat_blocks, tile_blocks, cell_blocks, spread_blocks))
    latent = latent_sum.astype(jnp.bfloat16)
    basis = basis_table(M, G, jnp.arange(G, dtype=jnp.int32))
    cube = latent.astype(jnp.float32).reshape(G, G, G, C)
    along_z = jnp.einsum('kz,xyzc->xykc', basis, cube, precision=highest)
    along_y = jnp.einsum('jy,xykc->xjkc', basis, along_z, precision=highest)
    spectrum = jnp.einsum('ix,xjkc->jikc', basis, along_y, precision=highest)
    spectrum = spectrum.reshape(M, M * M, C).astype(jnp.bfloat16)

    def mix_row(pair):
        spec_row, weight_row = pair
        return jnp.einsum('mc,mco->mo', spec_row.astype(jnp.float32), weight_row.astype(jnp.float32), precision=highest).astype(jnp.bfloat16)
    mixed = lax.map(mix_row, (spectrum, spectral_weight))
    mixed_cube = mixed.astype(jnp.float32).reshape(M, M, M, C)
    inv_z = jnp.einsum('kz,jikc->jizc', basis, mixed_cube, precision=highest)
    inv_x = jnp.einsum('ix,jizc->jxzc', basis, inv_z, precision=highest)
    inverse = jnp.einsum('jy,jxzc->xyzc', basis, inv_x, precision=highest)
    skip = jnp.dot(latent, skip_weight, preferred_element_type=jnp.float32)
    latent_out = jax.nn.gelu(inverse.reshape(G * G * G, C) + skip).astype(jnp.bfloat16)

    def read_step(carry, block):
        tile_block, cell_block, read_block = block
        rows = latent_out[global_cell(tile_block, cell_block)]
        gathered = (read_block[:, None] * rows.astype(jnp.float32)).astype(jnp.bfloat16)
        hidden = jax.nn.gelu(jnp.dot(gathered, hidden_weight, preferred_element_type=jnp.float32)).astype(jnp.bfloat16)
        result = jnp.dot(hidden, output_weight, preferred_element_type=jnp.float32).astype(jnp.bfloat16)
        return (carry, result)
    carry_out, results = lax.scan(read_step, jnp.zeros((), jnp.float32), (tile_blocks, cell_blocks, read_blocks))
    return results.reshape(POINTS, C)
```

```python
import functools
import math

import jax
import jax.numpy as jnp
import numpy as np
from jax import lax
from jax.experimental import pallas as pl
from jax.experimental.pallas import tpu as pltpu
from jax.sharding import PartitionSpec as P

G = 64
LANES = 128
F32 = jnp.float32
BF16 = jnp.bfloat16
MESH = pl.DeviceIdType.MESH


def basis_np(modes, grid):
    k = np.arange(modes)[:, None]
    half = modes // 2
    freq = np.where(k < half, k, k - half + 1).astype(np.float64)
    phase = 2.0 * math.pi * freq * np.arange(grid)[None, :] / grid
    wave = np.where(k < half, np.cos(phase), np.sin(phase))
    norm = np.where(k == 0, math.sqrt(1.0 / grid), math.sqrt(2.0 / grid))
    return (wave * norm).astype(np.float32)


def split_table(table):
    high = table.astype(BF16)
    low = (table - high.astype(np.float32)).astype(BF16)
    return np.concatenate([high, low], axis=0)


def dot(a, b):
    return jnp.dot(a, b, preferred_element_type=F32)


def rows_of(block, *shape):
    if any(size % 16 for size in (block.shape[-2], shape[-2])):
        return block.astype(F32).reshape(shape).astype(BF16)
    return block.reshape(shape)


def hot_rows(values, points):
    lane = lax.broadcasted_iota(jnp.int32, (2 * G, points), 0) % G
    return (lane.astype(F32) == values).astype(F32).astype(BF16)


def hot_columns(values, points):
    lane = lax.broadcasted_iota(jnp.int32, (points, 2 * G), 1) % G
    return (lane.astype(F32) == values).astype(F32).astype(BF16)


def layer_kernel(
    sizes,
    info_ref, feat_ref, wm_ref, ws_ref, wh_ref, wo_ref, txr_ref, tyr_ref, tzr_ref, txc_ref, tyc_ref, tzc_ref,
    spec_hbm, out_ref,
    spec, slots, cols, message, plane, second, plane_c, second_c, total,
    send, recv, back, ret, wsend, wrecv, wrow,
    part, from_core, from_quad, quad, from_line, mixed, whole,
    spec_sem, where_s, where_r, rows_s, rows_r, ret_s, ret_r,
    core_s, core_r, quad_s, quad_r, line_s, line_r,
    gline_s, gline_r, gquad_s, gquad_r, gcore_s, gcore_r,
):
    na, nb, cap, modes_y, share = sizes
    n = na * nb
    naz, nbx = na // 2, nb // 2
    points, width = feat_ref.shape
    pairs = txr_ref.shape[0]
    modes = modes_y * nb
    a = lax.axis_index("aa")
    b = lax.axis_index("ba")
    me = a * nb + b
    az, ay, bx, bc = a // 2, a % 2, b // 2, b % 2

    def remote(src, dst, send_sem, recv_sem, to_a, to_b):
        return pltpu.make_async_remote_copy(
            src_ref=src, dst_ref=dst, send_sem=send_sem, recv_sem=recv_sem,
            device_id={"aa": to_a, "ba": to_b}, device_id_type=MESH,
        )

    spec_copy = pltpu.make_async_copy(spec_hbm, spec, spec_sem)
    spec_copy.start()
    barrier = pltpu.get_barrier_semaphore()

    def greet(k, _):
        peer = (me + k) % n
        pl.semaphore_signal(
            barrier, inc=1, device_id={"aa": peer // nb, "ba": peer % nb}, device_id_type=MESH
        )
        return 0

    lax.fori_loop(1, n, greet, 0)

    step = 256
    upper = (
        lax.broadcasted_iota(jnp.int32, (step, step), 0) <= lax.broadcasted_iota(jnp.int32, (step, step), 1)
    ).astype(F32).astype(BF16)
    carry = jnp.zeros((n, 1), F32)
    tile_at = lax.broadcasted_iota(jnp.int32, (n, step), 0).astype(F32)
    rank_at = lax.broadcasted_iota(jnp.int32, (LANES, step), 0).astype(F32)
    found = jnp.zeros((3 * n, LANES), F32)
    for start in range(0, points, step):
        piece = slice(start, start + step)
        tiles = info_ref[0:1, piece]
        hot = (tile_at == tiles).astype(F32)
        counts = dot(hot.astype(BF16), upper) + carry
        rank = jnp.sum(counts * hot, axis=0, keepdims=True) - 1.0
        slots[:, piece] = tiles * cap + rank
        carry = carry + jnp.sum(hot, axis=1, keepdims=True)
        marks = jnp.concatenate([hot * info_ref[1:2, piece], hot * info_ref[2:3, piece], hot], axis=0).astype(BF16)
        ranks = (rank_at == rank).astype(F32).astype(BF16)
        found = found + lax.dot_general(marks, ranks, (((1,), (1,)), ((), ())), preferred_element_type=F32)
    where = found[:n] * G + found[n : 2 * n] + (found[2 * n :] - 1.0)
    for tile in range(n):
        wsend[tile] = where[tile : tile + 1, :]
    for start in range(0, points, LANES):
        piece = slice(start, start + LANES)
        both = jnp.concatenate([slots[:, piece], info_ref[1:8, piece]], axis=0)
        cols[piece, :] = both.T

    message[...] = (cols[:, 6:7] * dot(feat_ref[...], wm_ref[...])).astype(BF16)

    pl.semaphore_wait(barrier, n - 1)

    group = nb * cap
    own = lax.broadcasted_iota(jnp.int32, (group, points), 0).astype(F32)

    def row_copy(src, dst, sem_s, sem_r, to_a, to_b):
        return remote(src.at[to_a * nb + to_b], dst.at[me], sem_s.at[to_a * nb + to_b], sem_r.at[me], to_a, to_b)

    def pack_step(i, _):
        to_a = (a + naz + i) % na
        base = (to_a * group).astype(F32)
        hot = (own == slots[...] - base).astype(F32).astype(BF16)
        rows = dot(hot, message[...])
        for to_b in range(nb):
            dest = to_a * nb + to_b
            send[dest] = rows[to_b * cap : (to_b + 1) * cap].astype(BF16)

            @pl.when(dest != me)
            def _():
                row_copy(wsend, wrecv, where_s, where_r, to_a, to_b).start()
                row_copy(send, recv, rows_s, rows_r, to_a, to_b).start()

        return 0

    lax.fori_loop(0, na, pack_step, 0)
    recv[me] = send[me]
    wrecv[me] = wsend[me]

    plane[...] = dot(txr_ref[...], hot_rows(info_ref[3:4, :], points)) * dot(
        tzr_ref[...], hot_rows(info_ref[5:6, :], points)
    )
    second[...] = dot(tyr_ref[...], hot_rows(info_ref[4:5, :], points))

    def forward(to_b):
        def one(jj, _):
            scaled = (plane[...] * second[pl.ds(to_b * modes_y + jj, 1), :]).astype(BF16)
            result = dot(scaled, message[...])
            part[to_b, jj] = result.reshape(2, naz, share, width).astype(BF16)
            return 0

        lax.fori_loop(0, modes_y, one, 0)

    def core_copy(to_x):
        return remote(
            part.at[to_x * 2 + (1 - bc)], from_core.at[to_x], core_s.at[to_x], core_r.at[to_x], a, bx * 2 + (1 - bc)
        )

    def quad_copy(kx, ky):
        to_x, to_y = (bx + kx) % nbx, (ay + ky) % 2
        k = kx * 2 + ky
        return remote(
            part.at[to_x * 2 + bc, :, to_y], from_quad.at[k], quad_s.at[k], quad_r.at[k],
            az * 2 + to_y, to_x * 2 + bc,
        )

    def line_copy(k):
        to_z = (az + k) % naz
        return remote(quad.at[:, to_z], from_line.at[k], line_s.at[k], line_r.at[k], to_z * 2 + ay, b)

    for kx in range(nbx):
        to_x = (bx + 1 + kx) % nbx
        forward(to_x * 2 + (1 - bc))
        core_copy(to_x).start()
    for kx in range(nbx):
        to_x = (bx + 1 + kx) % nbx
        forward(to_x * 2 + bc)
        core_copy(to_x).wait_recv()
        part[to_x * 2 + bc] = (part[to_x * 2 + bc].astype(F32) + from_core[to_x].astype(F32)).astype(BF16)
        for ky in (1, 0):
            k = (1 + kx) % nbx
            if (k, ky) != (0, 0):
                quad_copy(k, ky).start()

    plane_c[...] = dot(hot_columns(cols[:, 3:4], points), txc_ref[...]) * dot(
        hot_columns(cols[:, 5:6], points), tzc_ref[...]
    )
    second_c[...] = dot(hot_columns(cols[:, 4:5], points), tyc_ref[...])

    sums = part[b, :, ay].astype(F32)
    for kx in range(nbx):
        for ky in range(2):
            if (kx, ky) != (0, 0):
                quad_copy(kx, ky).wait_recv()
                sums = sums + from_quad[kx * 2 + ky].astype(F32)
    quad[...] = sums.astype(BF16)
    for k in range(1, naz):
        line_copy(k).start()
    spec_copy.wait()
    sums = quad[:, az].astype(F32)
    for k in range(1, naz):
        line_copy(k).wait_recv()
        sums = sums + from_line[k].astype(F32)
    mixed[...] = sums.reshape(modes_y * share, width)

    row_at = lax.broadcasted_iota(jnp.int32, (8, width), 0)

    def mix_step(i, _):
        rows = mixed[pl.ds(pl.multiple_of(i * 8, 8), 8), :].astype(BF16)
        out = jnp.zeros((8, width), F32)
        for r in range(8):
            out = jnp.where(row_at == r, dot(rows, spec[i * 8 + r]), out)
        mixed[pl.ds(pl.multiple_of(i * 8, 8), 8), :] = out
        return 0

    lax.fori_loop(0, modes_y * share // 8, mix_step, 0)
    whole[b, :, ay, az] = mixed[...].reshape(modes_y, share, width).astype(BF16)

    def gline_copy(k, at_z):
        to_z = (az + k) % naz
        here = whole.at[b, :, ay, at_z]
        return remote(here, here, gline_s.at[k], gline_r.at[k], to_z * 2 + ay, b)

    def gquad_copy(kx, ky, at_x, at_y):
        to_x, to_y = (bx + kx) % nbx, (ay + ky) % 2
        k = kx * 2 + ky
        here = whole.at[at_x * 2 + bc, :, at_y]
        return remote(here, here, gquad_s.at[k], gquad_r.at[k], az * 2 + to_y, to_x * 2 + bc)

    def gcore_copy(at_x, at_c):
        here = whole.at[at_x * 2 + at_c]
        return remote(here, here, gcore_s.at[at_x], gcore_r.at[at_x], a, bx * 2 + (1 - bc))

    for k in range(1, naz):
        gline_copy(k, az).start()

    def arrived(i, _):
        src = (me + i) % n
        row_copy(wsend, wrecv, where_s, where_r, src // nb, src % nb).wait_send()
        row_copy(send, recv, rows_s, rows_r, src // nb, src % nb).wait_send()
        remote(wsend.at[src], wrecv.at[src], where_s.at[src], where_r.at[src], src // nb, src % nb).wait_recv()
        remote(send.at[src], recv.at[src], rows_s.at[src], rows_r.at[src], src // nb, src % nb).wait_recv()
        return 0

    lax.fori_loop(1, n, arrived, 0)
    for tile in range(n):
        wrow[:, tile * cap : (tile + 1) * cap] = wrecv[tile][:, :cap]
    diagonal = lax.broadcasted_iota(jnp.int32, (cap, LANES), 0) == lax.broadcasted_iota(jnp.int32, (cap, LANES), 1)

    def merge_step(i, _):
        to_a = (a + naz + i) % na
        column = jnp.concatenate(
            [
                jnp.sum(jnp.where(diagonal, wrecv[to_a * nb + to_b], 0.0), axis=1, keepdims=True)
                for to_b in range(nb)
            ],
            axis=0,
        )
        same = (column == wrow[...]).astype(F32).astype(BF16)
        rows = dot(same, rows_of(recv[...], n * cap, width))
        for to_b in range(nb):
            dest = to_a * nb + to_b
            back[dest] = rows[to_b * cap : (to_b + 1) * cap].astype(BF16)

            @pl.when(dest != me)
            def _():
                row_copy(back, ret, ret_s, ret_r, to_a, to_b).start()

        return 0

    half = na // 2
    lax.fori_loop(0, half // 2, merge_step, 0)
    for k in range(1, naz):
        gline_copy(k, (az + naz - k) % naz).wait_recv()
    for kx in range(nbx):
        for ky in range(2):
            if (kx, ky) != (0, 0):
                gquad_copy(kx, ky, bx, ay).start()
    lax.fori_loop(half // 2, na, merge_step, 0)
    ret[me] = back[me]
    for kx in range(nbx):
        for ky in range(2):
            if (kx, ky) != (0, 0):
                gquad_copy(kx, ky, (bx + nbx - kx) % nbx, (ay + ky) % 2).wait_recv()
    for at_x in range(nbx):
        gcore_copy(at_x, bc).start()

    block = 256

    def inverse(at_b, first):
        part_b = rows_of(whole[at_b].reshape(modes_y, pairs // share, share, width), modes_y * pairs, width)

        def one(i, _):
            here = pl.ds(pl.multiple_of(i * block, block), block)
            base = plane_c[here, :]
            table = second_c[here, :]
            lane = lax.broadcasted_iota(jnp.int32, (block, modes), 1)
            scaled = []
            for jj in range(modes_y):
                factor = jnp.sum(jnp.where(lane == at_b * modes_y + jj, table, 0.0), axis=1, keepdims=True)
                scaled.append((base * factor).astype(BF16))
            value = dot(jnp.concatenate(scaled, axis=1), part_b)
            total[here, :] = value if first else total[here, :] + value
            return 0

        lax.fori_loop(0, points // block, one, 0)

    for at_x in range(nbx):
        inverse(at_x * 2 + bc, at_x == 0)
    for at_x in range(nbx):
        gcore_copy(at_x, 1 - bc).wait_recv()
        inverse(at_x * 2 + (1 - bc), False)

    def returned(i, _):
        src = (me + i) % n
        row_copy(back, ret, ret_s, ret_r, src // nb, src % nb).wait_send()
        remote(back.at[src], ret.at[src], ret_s.at[src], ret_r.at[src], src // nb, src % nb).wait_recv()
        return 0

    lax.fori_loop(1, n, returned, 0)

    def decode(i, _):
        here = pl.ds(pl.multiple_of(i * block, block), block)
        lane = lax.broadcasted_iota(jnp.int32, (block, n * cap), 1).astype(F32)
        hot = (lane == cols[here, 0:1]).astype(F32).astype(BF16)
        latent = dot(hot, rows_of(ret[...], n * cap, width)).astype(BF16)
        latent_out = jax.nn.gelu(total[here, :] + dot(latent, ws_ref[...])).astype(BF16)
        gathered = (cols[here, 7:8] * latent_out.astype(F32)).astype(BF16)
        hidden = jax.nn.gelu(dot(gathered, wh_ref[...])).astype(BF16)
        out_ref[here, :] = dot(hidden, wo_ref[...]).astype(BF16)
        return 0

    lax.fori_loop(0, points // block, decode, 0)

    for to_x in range(nbx):
        core_copy(to_x).wait_send()
        gcore_copy(to_x, bc).wait_send()
    for kx in range(nbx):
        for ky in range(2):
            if (kx, ky) != (0, 0):
                quad_copy(kx, ky).wait_send()
                gquad_copy(kx, ky, bx, ay).wait_send()
    for k in range(1, naz):
        line_copy(k).wait_send()
        gline_copy(k, az).wait_send()


def per_device(
    features,
    tile_ids,
    cell_ids,
    spread_weight,
    read_weight,
    message_weight,
    skip_weight,
    spectral_weight,
    hidden_weight,
    output_weight,
):
    points, width = features.shape
    na = lax.axis_size("aa")
    nb = lax.axis_size("ba")
    n = na * nb
    cap = 3 * points // (2 * n)
    tile_x = G // na
    tile_y = G // nb
    modes_y, share = spectral_weight.shape[0], spectral_weight.shape[1]
    modes = modes_y * nb
    pairs = share * na
    naz, nbx = na // 2, nb // 2

    order = np.arange(pairs).reshape(naz, 2, share).transpose(1, 0, 2).reshape(pairs)
    basis = basis_np(modes, G)
    tx = split_table(np.repeat(basis, modes, axis=0)[order].T)
    tz = split_table(np.tile(basis, (modes, 1))[order].T)
    ty = split_table(basis.T)
    tables = [jnp.asarray(np.ascontiguousarray(t.T)) for t in (tx, ty, tz)] + [jnp.asarray(t) for t in (tx, ty, tz)]

    targets = tile_ids[:, 0]
    high, low = cell_ids // G, cell_ids % G
    x = targets // nb * tile_x + cell_ids // (tile_y * G)
    y = targets % nb * tile_y + high % tile_y
    info = jnp.stack(
        [targets.astype(F32), high.astype(F32), low.astype(F32), x.astype(F32), y.astype(F32), low.astype(F32),
         spread_weight, read_weight]
    )
    spec = spectral_weight.reshape(modes_y * share, width, width)

    vmem = pl.BlockSpec(memory_space=pltpu.VMEM)
    dma = pltpu.SemaphoreType.DMA
    return pl.pallas_call(
        functools.partial(layer_kernel, (na, nb, cap, modes_y, share)),
        in_specs=[vmem] * 12 + [pl.BlockSpec(memory_space=pl.ANY)],
        out_specs=vmem,
        out_shape=jax.ShapeDtypeStruct((points, width), BF16),
        scratch_shapes=[
            pltpu.VMEM((modes_y * share, width, width), BF16),
            pltpu.VMEM((1, points), F32),
            pltpu.VMEM((points, 8), F32),
            pltpu.VMEM((points, width), BF16),
            pltpu.VMEM((pairs, points), F32),
            pltpu.VMEM((modes, points), F32),
            pltpu.VMEM((points, pairs), F32),
            pltpu.VMEM((points, modes), F32),
            pltpu.VMEM((points, width), F32),
            pltpu.VMEM((n, cap, width), BF16),
            pltpu.VMEM((n, cap, width), BF16),
            pltpu.VMEM((n, cap, width), BF16),
            pltpu.VMEM((n, cap, width), BF16),
            pltpu.VMEM((n, 1, LANES), F32),
            pltpu.VMEM((n, 1, LANES), F32),
            pltpu.VMEM((1, n * cap), F32),
            pltpu.VMEM((nb, modes_y, 2, naz, share, width), BF16),
            pltpu.VMEM((nbx, modes_y, 2, naz, share, width), BF16),
            pltpu.VMEM((2 * nbx, modes_y, naz, share, width), BF16),
            pltpu.VMEM((modes_y, naz, share, width), BF16),
            pltpu.VMEM((naz, modes_y, share, width), BF16),
            pltpu.VMEM((modes_y * share, width), F32),
            pltpu.VMEM((nb, modes_y, 2, naz, share, width), BF16),
            dma, dma((n,)), dma((n,)), dma((n,)), dma((n,)), dma((n,)), dma((n,)),
            dma((nbx,)), dma((nbx,)), dma((2 * nbx,)), dma((2 * nbx,)), dma((naz,)), dma((naz,)),
            dma((naz,)), dma((naz,)), dma((2 * nbx,)), dma((2 * nbx,)), dma((nbx,)), dma((nbx,)),
        ],
        compiler_params=pltpu.CompilerParams(
            collective_id=0, has_side_effects=True, vmem_limit_bytes=62 * 1024 * 1024
        ),
        name="layer",
    )(info, features, message_weight, skip_weight, hidden_weight, output_weight, *tables, spec)


def solution(mesh):
    placed = (
        P(("aa", "ba"), None),
        P(("aa", "ba"), None),
        P(("aa", "ba")),
        P(("aa", "ba")),
        P(("aa", "ba")),
        P(),
        P(),
        P("ba", "aa", None, None),
        P(),
        P(),
    )
    return jax.shard_map(
        per_device, mesh=mesh, in_specs=placed, out_specs=P(("aa", "ba"), None), check_vma=False
    )
```

```python
import functools
import math

import jax
import jax.numpy as jnp
import numpy as np
from jax import lax
from jax.experimental import pallas as pl
from jax.experimental.pallas import tpu as pltpu
from jax.sharding import PartitionSpec as P

G = 64
LANES = 128
F32 = jnp.float32
BF16 = jnp.bfloat16
PACE = (4, 4, 0, 0, 18)
MESH = pl.DeviceIdType.MESH


def FAR(size):
    return [(size // 2 + i) % size for i in range(size) if (size // 2 + i) % size]


def basis_np(modes, grid):
    k = np.arange(modes)[:, None]
    half = modes // 2
    freq = np.where(k < half, k, k - half + 1).astype(np.float64)
    phase = 2.0 * math.pi * freq * np.arange(grid)[None, :] / grid
    wave = np.where(k < half, np.cos(phase), np.sin(phase))
    norm = np.where(k == 0, math.sqrt(1.0 / grid), math.sqrt(2.0 / grid))
    return (wave * norm).astype(np.float32)


def split_table(table):
    high = table.astype(BF16)
    low = (table - high.astype(np.float32)).astype(BF16)
    return np.concatenate([high, low], axis=0)


def dot(a, b):
    return jnp.dot(a, b, preferred_element_type=F32)


def rows_of(block, *shape):
    if any(size % 16 for size in (block.shape[-2], shape[-2])):
        return block.astype(F32).reshape(shape).astype(BF16)
    return block.reshape(shape)


def hot_rows(values, points):
    lane = lax.broadcasted_iota(jnp.int32, (2 * G, points), 0) % G
    return (lane.astype(F32) == values).astype(F32).astype(BF16)


def hot_columns(values, points):
    lane = lax.broadcasted_iota(jnp.int32, (points, 2 * G), 1) % G
    return (lane.astype(F32) == values).astype(F32).astype(BF16)


def layer_kernel(
    sizes,
    tile_ref, cell_ref, spread_ref, read_ref, feat_ref, wm_ref, ws_ref, wh_ref, txr_ref, tyr_ref, tzr_ref, txc_ref, tyc_ref, tzc_ref,
    spec_hbm, out_ref,
    spec, info, slots, cols, message, plane, second, plane_c, second_c, total, latent,
    send, recv, back, ret, wsend, wrecv, wrow,
    part, from_core, from_quad, quad, from_line, mixed, whole,
    spec_sem, where_s, where_r, rows_s, rows_r, ret_s, ret_r,
    core_s, core_r, quad_s, quad_r, line_s, line_r,
    gline_s, gline_r, gquad_s, gquad_r, gcore_s, gcore_r,
):
    na, nb, cap, modes_y, share = sizes
    n = na * nb
    naz, nbx = na // 2, nb // 2
    points, width = feat_ref.shape
    pairs = txr_ref.shape[0]
    modes = modes_y * nb
    a = lax.axis_index("aa")
    b = lax.axis_index("ba")
    me = a * nb + b
    az, ay, bx, bc = a // 2, a % 2, b // 2, b % 2
    turn = 1 - 2 * (az // (naz // 2))

    def remote(src, dst, send_sem, recv_sem, to_a, to_b):
        return pltpu.make_async_remote_copy(
            src_ref=src, dst_ref=dst, send_sem=send_sem, recv_sem=recv_sem,
            device_id={"aa": to_a, "ba": to_b}, device_id_type=MESH,
        )


    spec_copy = pltpu.make_async_copy(spec_hbm, spec, spec_sem)
    spec_copy.start()
    barrier = pltpu.get_barrier_semaphore()

    def greet(k, _):
        peer = (me + k) % n
        pl.semaphore_signal(
            barrier, inc=1, device_id={"aa": peer // nb, "ba": peer % nb}, device_id_type=MESH
        )
        return 0

    lax.fori_loop(1, n, greet, 0)


    tile = tile_ref[...].astype(F32)
    cell = cell_ref[...].astype(F32)
    tile_x, tile_y = G // na, G // nb
    row = jnp.floor((tile + 0.5) * (1.0 / nb))
    high = jnp.floor((cell + 0.5) * (1.0 / G))
    deep = jnp.floor((high + 0.5) * (1.0 / tile_y))
    low = cell - high * G
    info[0:1, :] = tile
    info[1:2, :] = high
    info[2:3, :] = low
    info[3:4, :] = row * tile_x + deep
    info[4:5, :] = (tile - row * nb) * tile_y + (high - deep * tile_y)
    info[5:6, :] = low
    info[6:7, :] = spread_ref[...]
    info[7:8, :] = read_ref[...]

    step = 256
    upper = (
        lax.broadcasted_iota(jnp.int32, (step, step), 0) <= lax.broadcasted_iota(jnp.int32, (step, step), 1)
    ).astype(F32).astype(BF16)
    carry = jnp.zeros((n, 1), F32)
    tile_at = lax.broadcasted_iota(jnp.int32, (n, step), 0).astype(F32)
    rank_at = lax.broadcasted_iota(jnp.int32, (LANES, step), 0).astype(F32)
    found = jnp.zeros((3 * n, LANES), F32)
    for start in range(0, points, step):
        piece = slice(start, start + step)
        tiles = info[0:1, piece]
        hot = (tile_at == tiles).astype(F32)
        counts = dot(hot.astype(BF16), upper) + carry
        rank = jnp.sum(counts * hot, axis=0, keepdims=True) - 1.0
        slots[:, piece] = tiles * cap + rank
        carry = carry + jnp.sum(hot, axis=1, keepdims=True)
        marks = jnp.concatenate([hot * info[1:2, piece], hot * info[2:3, piece], hot], axis=0).astype(BF16)
        ranks = (rank_at == rank).astype(F32).astype(BF16)
        found = found + lax.dot_general(marks, ranks, (((1,), (1,)), ((), ())), preferred_element_type=F32)
    where = found[:n] * G + found[n : 2 * n] + (found[2 * n :] - 1.0)
    for tile in range(n):
        wsend[tile] = where[tile : tile + 1, :]
    for start in range(0, points, LANES):
        piece = slice(start, start + LANES)
        both = jnp.concatenate([slots[:, piece], info[1:8, piece]], axis=0)
        cols[piece, :] = both.T

    message[...] = (cols[:, 6:7] * dot(feat_ref[...], wm_ref[...])).astype(BF16)


    pl.semaphore_wait(barrier, n - 1)


    block = 512

    group = nb * cap
    own = lax.broadcasted_iota(jnp.int32, (group, points), 0).astype(F32)

    def row_copy(src, dst, sem_s, sem_r, to_a, to_b):
        return remote(src.at[to_a * nb + to_b], dst.at[me], sem_s.at[to_a * nb + to_b], sem_r.at[me], to_a, to_b)

    def peer(dz, dy, dx, dc):
        return (az + turn * dz + naz) % naz * 2 + (ay + dy) % 2, (bx + dx) % nbx * 2 + (bc + dc) % 2

    def send_rows(to_a, to_b):
        row_copy(wsend, wrecv, where_s, where_r, to_a, to_b).start()
        row_copy(send, recv, rows_s, rows_r, to_a, to_b).start()

    def pack(dy):
        def one(i, _):
            dz = (naz // 2 + i) % naz
            to_a = (az + turn * dz + naz) % naz * 2 + (ay + dy) % 2
            base = (to_a * group).astype(F32)
            hot = (own == slots[...] - base).astype(F32).astype(BF16)
            rows = dot(hot, message[...])
            for to_b in range(nb):
                send[to_a * nb + to_b] = rows[to_b * cap : (to_b + 1) * cap].astype(BF16)
            if dy == 0:
                for dc in range(2):
                    to_b = bx * 2 + (bc + dc) % 2

                    @pl.when(to_a * nb + to_b != me)
                    def _():
                        send_rows(to_a, to_b)

            return 0

        lax.fori_loop(0, naz, one, 0)

    sides = [(dx, dy) for dx in range(nbx) for dy in range(2) if (dx, dy) != (0, 0)]
    far = [(dz, dy, dx, dc) for dz in FAR(naz) for dc in range(2) for dx, dy in sides]
    near = [(0, dy, dx, dc) for dc in range(2) for dx, dy in sides]
    pack(0)
    pack(1)
    for offsets in near:
        send_rows(*peer(*offsets))
    recv[me] = send[me]
    wrecv[me] = wsend[me]


    plane[...] = dot(txr_ref[...], hot_rows(info[3:4, :], points)) * dot(
        tzr_ref[...], hot_rows(info[5:6, :], points)
    )
    second[...] = dot(tyr_ref[...], hot_rows(info[4:5, :], points))

    def forward(to_b):
        def one(jj, _):
            scaled = (plane[...] * second[pl.ds(to_b * modes_y + jj, 1), :]).astype(BF16)
            result = dot(scaled, message[...])
            part[to_b, jj] = result.reshape(2, naz, share, width).astype(BF16)
            return 0

        lax.fori_loop(0, modes_y, one, 0)

    def core_copy(to_x):
        return remote(
            part.at[to_x * 2 + (1 - bc)], from_core.at[to_x], core_s.at[to_x], core_r.at[to_x], a, bx * 2 + (1 - bc)
        )

    def quad_copy(kx, ky):
        to_x, to_y = (bx + kx) % nbx, (ay + ky) % 2
        k = kx * 2 + ky
        return remote(
            part.at[to_x * 2 + bc, :, to_y], from_quad.at[k], quad_s.at[k], quad_r.at[k],
            az * 2 + to_y, to_x * 2 + bc,
        )

    def line_copy(k, inward=False):
        to_z = (az + turn * k + naz) % naz
        at_z = to_z if inward else az
        return remote(quad.at[:, to_z], from_line.at[at_z], line_s.at[to_z], line_r.at[at_z], to_z * 2 + ay, b)

    paced = iter(far)

    def pace(count):
        for offsets in [o for _, o in zip(range(count), paced)]:
            send_rows(*peer(*offsets))

    early = iter(PACE)
    for kx in range(nbx):
        to_x = (bx + 1 + kx) % nbx
        pace(len(far) * next(early) // 18)
        forward(to_x * 2 + (1 - bc))
        core_copy(to_x).start()
    for kx in range(nbx):
        to_x = (bx + 1 + kx) % nbx
        pace(len(far) * next(early) // 18)
        forward(to_x * 2 + bc)
        core_copy(to_x).wait_recv()
        part[to_x * 2 + bc] = (part[to_x * 2 + bc].astype(F32) + from_core[to_x].astype(F32)).astype(BF16)
        for ky in (1, 0):
            k = (1 + kx) % nbx
            if (k, ky) != (0, 0):
                quad_copy(k, ky).start()
    pace(len(far) * next(early) // 18)


    def position(i, _):
        here = pl.ds(pl.multiple_of(i * block, block), block)
        plane_c[here, :] = (
            dot(hot_columns(cols[here, 3:4], block), txc_ref[...])
            * dot(hot_columns(cols[here, 5:6], block), tzc_ref[...])
        ).astype(BF16)
        hot_y = hot_columns(cols[here, 4:5], block)
        for j in range(modes):
            second_c[j, here, :] = dot(hot_y, tyc_ref[j]).astype(BF16)
        return 0

    lax.fori_loop(0, points // block, position, 0)


    sums = part[b, :, ay].astype(F32)
    for kx in range(nbx):
        for ky in range(2):
            if (kx, ky) != (0, 0):
                quad_copy(kx, ky).wait_recv()
                sums = sums + from_quad[kx * 2 + ky].astype(F32)
    quad[...] = sums.astype(BF16)

    for k in FAR(naz):
        line_copy(k).start()
    pace(len(far))
    def gline_copy(k, inward=False):
        to_z = (az + turn * k + naz) % naz
        at_z = to_z if inward else az
        here = whole.at[b, :, ay, at_z]
        return remote(here, here, gline_s.at[to_z], gline_r.at[at_z], to_z * 2 + ay, b)

    def gquad_copy(kx, ky, at_x, at_y):
        to_x, to_y = (bx + kx) % nbx, (ay + ky) % 2
        k = kx * 2 + ky
        here = whole.at[at_x * 2 + bc, :, at_y]
        return remote(here, here, gquad_s.at[k], gquad_r.at[k], az * 2 + to_y, to_x * 2 + bc)

    def gcore_copy(k, at_x, at_y, at_c):
        here = whole.at[at_x * 2 + at_c, :, at_y]
        return remote(here, here, gcore_s.at[k], gcore_r.at[k], a, bx * 2 + (1 - bc))


    def arrived(i, _):
        src = (me + i) % n
        remote(wsend.at[src], wrecv.at[src], where_s.at[src], where_r.at[src], src // nb, src % nb).wait_recv()
        remote(send.at[src], recv.at[src], rows_s.at[src], rows_r.at[src], src // nb, src % nb).wait_recv()
        return 0

    lax.fori_loop(1, n, arrived, 0)

    for tile in range(n):
        wrow[:, tile * cap : (tile + 1) * cap] = wrecv[tile][:, :cap]
    diagonal = lax.broadcasted_iota(jnp.int32, (cap, LANES), 0) == lax.broadcasted_iota(jnp.int32, (cap, LANES), 1)

    def back_rows(to_a, to_b):
        row_copy(back, ret, ret_s, ret_r, to_a, to_b).start()

    def merge(dy, zero, count):
        def one(i, _):
            dz = (zero + i) % naz
            to_a = (az + turn * dz + naz) % naz * 2 + (ay + dy) % 2
            column = jnp.concatenate(
                [
                    jnp.sum(jnp.where(diagonal, wrecv[to_a * nb + to_b], 0.0), axis=1, keepdims=True)
                    for to_b in range(nb)
                ],
                axis=0,
            )
            same = (column == wrow[...]).astype(F32).astype(BF16)
            rows = dot(same, rows_of(recv[...], n * cap, width))
            for to_b in range(nb):
                back[to_a * nb + to_b] = rows[to_b * cap : (to_b + 1) * cap].astype(BF16)
            if dy == 0:
                for dc in range(2):
                    to_b = bx * 2 + (bc + dc) % 2

                    @pl.when(to_a * nb + to_b != me)
                    def _():
                        back_rows(to_a, to_b)

            return 0

        lax.fori_loop(0, count, one, 0)

    def far_back(first, last):
        for offsets in far[first:last]:
            back_rows(*peer(*offsets))

    merge(0, naz // 2, 1)
    merge(0, 0, 1)
    merge(1, 0, 1)
    for offsets in near:
        back_rows(*peer(*offsets))
    ret[me] = back[me]

    spec_copy.wait()
    sums = quad[:, az].astype(F32)
    for k in range(1, naz):
        line_copy(k, True).wait_recv()
        sums = sums + from_line[(az + turn * k + naz) % naz].astype(F32)
    mixed[...] = sums.reshape(modes_y * share, width)


    row_at = lax.broadcasted_iota(jnp.int32, (8, width), 0)

    def mix_step(i, _):
        rows = mixed[pl.ds(pl.multiple_of(i * 8, 8), 8), :].astype(BF16)
        out = jnp.zeros((8, width), F32)
        for r in range(8):
            out = jnp.where(row_at == r, dot(rows, spec[i * 8 + r]), out)
        mixed[pl.ds(pl.multiple_of(i * 8, 8), 8), :] = out
        return 0

    lax.fori_loop(0, modes_y * share // 8, mix_step, 0)
    whole[b, :, ay, az] = mixed[...].reshape(modes_y, share, width).astype(BF16)

    for k in FAR(naz):
        gline_copy(k).start()


    merge(0, naz // 2 + 1, naz - naz // 2 - 1)
    merge(0, 1, naz // 2 - 1)
    merge(1, 1, naz - 1)

    slab = 2 * nb

    def unpack(dz, first):

        at_z = (az + turn * dz + naz) % naz
        for q in range(slab):
            src = at_z * slab + q

            @pl.when(src != me)
            def _():
                remote(back.at[src], ret.at[src], ret_s.at[src], ret_r.at[src], src // nb, src % nb).wait_recv()


        rows = rows_of(ret[pl.ds(at_z * slab, slab)], slab * cap, width)
        base = (at_z * slab * cap).astype(F32)

        def one(i, _):
            here = pl.ds(pl.multiple_of(i * block, block), block)
            lane = lax.broadcasted_iota(jnp.int32, (block, slab * cap), 1).astype(F32) + base
            hot = (lane == cols[here, 0:1]).astype(F32).astype(BF16)
            value = dot(hot, rows)
            latent[here, :] = value if first else latent[here, :] + value
            return 0

        lax.fori_loop(0, points // block, one, 0)


    for k in range(1, naz):
        gline_copy(k, True).wait_recv()
    for kx in range(nbx):
        for ky in range(2):
            if (kx, ky) != (0, 0):
                gquad_copy(kx, ky, bx, ay).start()

    half = pairs // 2

    def inverse(at_b, at_y, first):
        part_b = rows_of(whole[at_b, :, at_y].reshape(modes_y, naz * share, width), modes_y * half, width)

        def one(i, _):
            here = pl.ds(pl.multiple_of(i * block, block), block)
            base = plane_c[here, pl.ds(pl.multiple_of(at_y * half, half), half)]
            scaled = [base * second_c[at_b * modes_y + jj, here, :] for jj in range(modes_y)]
            value = dot(jnp.concatenate(scaled, axis=1), part_b)
            total[here, :] = value if first else total[here, :] + value
            return 0

        lax.fori_loop(0, points // block, one, 0)

    def take(kx, ky):
        at_x, at_y = (bx + nbx - kx) % nbx, (ay + ky) % 2
        first = (kx, ky) == (0, 0)
        if not first:

            gquad_copy(kx, ky, at_x, at_y).wait_recv()

        gcore_copy(kx * 2 + ky, at_x, at_y, bc).start()
        inverse(at_x * 2 + bc, at_y, first)
        if first:
            far_back(0, len(far) // 3)

        gcore_copy(kx * 2 + ky, at_x, at_y, 1 - bc).wait_recv()

        inverse(at_x * 2 + (1 - bc), at_y, False)
        if first:
            far_back(len(far) // 3, len(far))

    take(0, 0)
    for dz in [0] + FAR(naz):

        unpack(dz, dz == 0)
    for dx, dy in sides:
        take(dx, dy)

    def left(i, _):
        src = (me + i) % n
        row_copy(back, ret, ret_s, ret_r, src // nb, src % nb).wait_send()
        row_copy(wsend, wrecv, where_s, where_r, src // nb, src % nb).wait_send()
        row_copy(send, recv, rows_s, rows_r, src // nb, src % nb).wait_send()
        return 0

    lax.fori_loop(1, n, left, 0)


    def decode(i, _):
        here = pl.ds(pl.multiple_of(i * block, block), block)
        latent_out = jax.nn.gelu(total[here, :] + dot(latent[here, :].astype(BF16), ws_ref[...])).astype(BF16)
        gathered = (cols[here, 7:8] * latent_out.astype(F32)).astype(BF16)
        out_ref[here, :] = jax.nn.gelu(dot(gathered, wh_ref[...])).astype(BF16)
        return 0

    lax.fori_loop(0, points // block, decode, 0)


    for to_x in range(nbx):
        core_copy(to_x).wait_send()
    for kx in range(nbx):
        for ky in range(2):
            gcore_copy(kx * 2 + ky, bx, ay, bc).wait_send()
            if (kx, ky) != (0, 0):
                quad_copy(kx, ky).wait_send()
                gquad_copy(kx, ky, bx, ay).wait_send()
    for k in range(1, naz):
        line_copy(k).wait_send()
        gline_copy(k).wait_send()


def per_device(
    features,
    tile_ids,
    cell_ids,
    spread_weight,
    read_weight,
    message_weight,
    skip_weight,
    spectral_weight,
    hidden_weight,
    output_weight,
):
    points, width = features.shape
    na = lax.axis_size("aa")
    nb = lax.axis_size("ba")
    n = na * nb
    cap = 3 * points // (2 * n)
    modes_y, share = spectral_weight.shape[0], spectral_weight.shape[1]
    modes = modes_y * nb
    pairs = share * na
    naz, nbx = na // 2, nb // 2

    order = np.arange(pairs).reshape(naz, 2, share).transpose(1, 0, 2).reshape(pairs)
    basis = basis_np(modes, G)
    tx = split_table(np.repeat(basis, modes, axis=0)[order].T)
    tz = split_table(np.tile(basis, (modes, 1))[order].T)
    ty = split_table(basis.T)
    tables = [jnp.asarray(np.ascontiguousarray(t.T)) for t in (tx, ty, tz)] + [
        jnp.asarray(t) for t in (tx, np.repeat(ty.T[:, :, None], pairs // 2, axis=2), tz)
    ]

    spec = spectral_weight.reshape(modes_y * share, width, width)

    vmem = pl.BlockSpec(memory_space=pltpu.VMEM)
    dma = pltpu.SemaphoreType.DMA
    hidden = pl.pallas_call(
        functools.partial(layer_kernel, (na, nb, cap, modes_y, share)),
        in_specs=[vmem] * 14 + [pl.BlockSpec(memory_space=pl.ANY)],
        out_specs=vmem,
        out_shape=jax.ShapeDtypeStruct((points, width), BF16),
        scratch_shapes=[
            pltpu.VMEM((modes_y * share, width, width), BF16),
            pltpu.VMEM((8, points), F32),
            pltpu.VMEM((1, points), F32),
            pltpu.VMEM((points, 8), F32),
            pltpu.VMEM((points, width), BF16),
            pltpu.VMEM((pairs, points), F32),
            pltpu.VMEM((modes, points), F32),
            pltpu.VMEM((points, pairs), BF16),
            pltpu.VMEM((modes, points, pairs // 2), BF16),
            pltpu.VMEM((points, width), F32),
            pltpu.VMEM((points, width), F32),
            pltpu.VMEM((n, cap, width), BF16),
            pltpu.VMEM((n, cap, width), BF16),
            pltpu.VMEM((n, cap, width), BF16),
            pltpu.VMEM((n, cap, width), BF16),
            pltpu.VMEM((n, 1, LANES), F32),
            pltpu.VMEM((n, 1, LANES), F32),
            pltpu.VMEM((1, n * cap), F32),
            pltpu.VMEM((nb, modes_y, 2, naz, share, width), BF16),
            pltpu.VMEM((nbx, modes_y, 2, naz, share, width), BF16),
            pltpu.VMEM((2 * nbx, modes_y, naz, share, width), BF16),
            pltpu.VMEM((modes_y, naz, share, width), BF16),
            pltpu.VMEM((naz, modes_y, share, width), BF16),
            pltpu.VMEM((modes_y * share, width), F32),
            pltpu.VMEM((nb, modes_y, 2, naz, share, width), BF16),
            dma, dma((n,)), dma((n,)), dma((n,)), dma((n,)), dma((n,)), dma((n,)),
            dma((nbx,)), dma((nbx,)), dma((2 * nbx,)), dma((2 * nbx,)), dma((naz,)), dma((naz,)),
            dma((naz,)), dma((naz,)), dma((2 * nbx,)), dma((2 * nbx,)), dma((2 * nbx,)), dma((2 * nbx,)),
        ],
        compiler_params=pltpu.CompilerParams(
            collective_id=0, has_side_effects=True, vmem_limit_bytes=62 * 1024 * 1024
        ),
        name="layer",
    )(
        tile_ids.reshape(1, points), cell_ids.reshape(1, points), spread_weight.reshape(1, points),
        read_weight.reshape(1, points), features, message_weight, skip_weight, hidden_weight, *tables, spec,
    )
    return dot(hidden, output_weight).astype(BF16)


def solution(mesh):
    placed = (
        P(("aa", "ba"), None),
        P(("aa", "ba"), None),
        P(("aa", "ba")),
        P(("aa", "ba")),
        P(("aa", "ba")),
        P(),
        P(),
        P("ba", "aa", None, None),
        P(),
        P(),
    )
    return jax.shard_map(
        per_device, mesh=mesh, in_specs=placed, out_specs=P(("aa", "ba"), None), check_vma=False
    )
```

```python
import functools
import math

import jax
import jax.numpy as jnp
import numpy as np
from jax import lax
from jax.experimental import pallas as pl
from jax.experimental.pallas import tpu as pltpu
from jax.sharding import PartitionSpec as P

G = 64
LANES = 128
F32 = jnp.float32
BF16 = jnp.bfloat16
PACE = (4, 4, 0, 0, 18)
MESH = pl.DeviceIdType.MESH


def FAR(size):
    return [(size // 2 + i) % size for i in range(size) if (size // 2 + i) % size]


def basis_np(modes, grid):
    k = np.arange(modes)[:, None]
    half = modes // 2
    freq = np.where(k < half, k, k - half + 1).astype(np.float64)
    phase = 2.0 * math.pi * freq * np.arange(grid)[None, :] / grid
    wave = np.where(k < half, np.cos(phase), np.sin(phase))
    norm = np.where(k == 0, math.sqrt(1.0 / grid), math.sqrt(2.0 / grid))
    return (wave * norm).astype(np.float32)


def split_table(table):
    high = table.astype(BF16)
    low = (table - high.astype(np.float32)).astype(BF16)
    return np.concatenate([high, low], axis=0)


def dot(a, b):
    return jnp.dot(a, b, preferred_element_type=F32)


def rows_of(block, *shape):
    if any(size % 16 for size in (block.shape[-2], shape[-2])):
        return block.astype(F32).reshape(shape).astype(BF16)
    return block.reshape(shape)


def hot_rows(values, points):
    lane = lax.broadcasted_iota(jnp.int32, (2 * G, points), 0) % G
    return (lane.astype(F32) == values).astype(F32).astype(BF16)


def hot_columns(values, points):
    lane = lax.broadcasted_iota(jnp.int32, (points, 2 * G), 1) % G
    return (lane.astype(F32) == values).astype(F32).astype(BF16)


def layer_kernel(
    sizes,
    tile_hbm, cell_hbm, spread_hbm, read_hbm, feat_hbm, wm_hbm, ws_hbm, wh_hbm, txr_hbm, tyr_hbm, tzr_hbm, txc_hbm, tyc_hbm, tzc_hbm,
    spec_hbm, out_ref,
    spec, info, slots, cols, message, plane, second, plane_c, second_c, total, latent,
    send, recv, back, ret, wsend, wrecv, wrow,
    part, from_core, from_quad, quad, from_line, mixed, whole,
    spec_sem, where_s, where_r, rows_s, rows_r, ret_s, ret_r,
    core_s, core_r, quad_s, quad_r, line_s, line_r,
    gline_s, gline_r, gquad_s, gquad_r, gcore_s, gcore_r, load_sem,
    tile_ref, cell_ref, spread_ref, read_ref, feat_ref, wm_ref, ws_ref, wh_ref, txr_ref, tyr_ref, tzr_ref, txc_ref, tyc_ref, tzc_ref,
):
    na, nb, cap, modes_y, share = sizes
    n = na * nb
    naz, nbx = na // 2, nb // 2
    points, width = feat_ref.shape
    pairs = txr_ref.shape[0]
    modes = modes_y * nb
    a = lax.axis_index("aa")
    b = lax.axis_index("ba")
    me = a * nb + b
    az, ay, bx, bc = a // 2, a % 2, b // 2, b % 2
    turn = 1 - 2 * (az // (naz // 2))

    def remote(src, dst, send_sem, recv_sem, to_a, to_b):
        return pltpu.make_async_remote_copy(
            src_ref=src, dst_ref=dst, send_sem=send_sem, recv_sem=recv_sem,
            device_id={"aa": to_a, "ba": to_b}, device_id_type=MESH,
        )


    loads = [
        pltpu.make_async_copy(src, dst, load_sem.at[i])
        for i, (src, dst) in enumerate([
            (tile_hbm, tile_ref), (cell_hbm, cell_ref), (spread_hbm, spread_ref), (read_hbm, read_ref),
            (feat_hbm, feat_ref), (wm_hbm, wm_ref), (ws_hbm, ws_ref), (wh_hbm, wh_ref), (txr_hbm, txr_ref),
            (tyr_hbm, tyr_ref), (tzr_hbm, tzr_ref), (txc_hbm, txc_ref), (tyc_hbm, tyc_ref), (tzc_hbm, tzc_ref),
        ])
    ]
    barrier = pltpu.get_barrier_semaphore()

    def greet(k, _):
        peer = (me + k) % n
        pl.semaphore_signal(
            barrier, inc=1, device_id={"aa": peer // nb, "ba": peer % nb}, device_id_type=MESH
        )
        return 0

    lax.fori_loop(1, n, greet, 0)
    for load in loads:
        load.start()
    spec_copy = pltpu.make_async_copy(spec_hbm, spec, spec_sem)
    spec_copy.start()


    for load in loads[:4]:
        load.wait()
    tile = tile_ref[...].astype(F32)
    cell = cell_ref[...].astype(F32)
    tile_x, tile_y = G // na, G // nb
    row = jnp.floor((tile + 0.5) * (1.0 / nb))
    high = jnp.floor((cell + 0.5) * (1.0 / G))
    deep = jnp.floor((high + 0.5) * (1.0 / tile_y))
    low = cell - high * G
    info[0:1, :] = tile
    info[1:2, :] = high
    info[2:3, :] = low
    info[3:4, :] = row * tile_x + deep
    info[4:5, :] = (tile - row * nb) * tile_y + (high - deep * tile_y)
    info[5:6, :] = low
    info[6:7, :] = spread_ref[...]
    info[7:8, :] = read_ref[...]

    step = 256
    upper = (
        lax.broadcasted_iota(jnp.int32, (step, step), 0) <= lax.broadcasted_iota(jnp.int32, (step, step), 1)
    ).astype(F32).astype(BF16)
    carry = jnp.zeros((n, 1), F32)
    tile_at = lax.broadcasted_iota(jnp.int32, (n, step), 0).astype(F32)
    rank_at = lax.broadcasted_iota(jnp.int32, (LANES, step), 0).astype(F32)
    found = jnp.zeros((3 * n, LANES), F32)
    for start in range(0, points, step):
        piece = slice(start, start + step)
        tiles = info[0:1, piece]
        hot = (tile_at == tiles).astype(F32)
        counts = dot(hot.astype(BF16), upper) + carry
        rank = jnp.sum(counts * hot, axis=0, keepdims=True) - 1.0
        slots[:, piece] = tiles * cap + rank
        carry = carry + jnp.sum(hot, axis=1, keepdims=True)
        marks = jnp.concatenate([hot * info[1:2, piece], hot * info[2:3, piece], hot], axis=0).astype(BF16)
        ranks = (rank_at == rank).astype(F32).astype(BF16)
        found = found + lax.dot_general(marks, ranks, (((1,), (1,)), ((), ())), preferred_element_type=F32)
    where = found[:n] * G + found[n : 2 * n] + (found[2 * n :] - 1.0)
    for tile in range(n):
        wsend[tile] = where[tile : tile + 1, :]
    for start in range(0, points, LANES):
        piece = slice(start, start + LANES)
        both = jnp.concatenate([slots[:, piece], info[1:8, piece]], axis=0)
        cols[piece, :] = both.T

    for load in loads[4:]:
        load.wait()
    message[...] = (cols[:, 6:7] * dot(feat_ref[...], wm_ref[...])).astype(BF16)


    pl.semaphore_wait(barrier, n - 1)


    block = 512

    group = nb * cap
    own = lax.broadcasted_iota(jnp.int32, (group, points), 0).astype(F32)

    def row_copy(src, dst, sem_s, sem_r, to_a, to_b):
        return remote(src.at[to_a * nb + to_b], dst.at[me], sem_s.at[to_a * nb + to_b], sem_r.at[me], to_a, to_b)

    def peer(dz, dy, dx, dc):
        return (az + turn * dz + naz) % naz * 2 + (ay + dy) % 2, (bx + dx) % nbx * 2 + (bc + dc) % 2

    def send_rows(to_a, to_b):
        row_copy(wsend, wrecv, where_s, where_r, to_a, to_b).start()
        row_copy(send, recv, rows_s, rows_r, to_a, to_b).start()

    def pack(dy):
        def one(i, _):
            dz = (naz // 2 + i) % naz
            to_a = (az + turn * dz + naz) % naz * 2 + (ay + dy) % 2
            base = (to_a * group).astype(F32)
            hot = (own == slots[...] - base).astype(F32).astype(BF16)
            rows = dot(hot, message[...])
            for to_b in range(nb):
                send[to_a * nb + to_b] = rows[to_b * cap : (to_b + 1) * cap].astype(BF16)
            if dy == 0:

                @pl.when(to_a != a)
                def _():
                    for dc in range(2):
                        send_rows(to_a, bx * 2 + (bc + dc) % 2)

            return 0

        lax.fori_loop(0, naz, one, 0)

    sides = [(dx, dy) for dx in range(nbx) for dy in range(2) if (dx, dy) != (0, 0)]
    far = [(dz, dy, dx, dc) for dz in FAR(naz) for dc in range(2) for dx, dy in sides]
    near = [(0, dy, dx, dc) for dc in range(2) for dx, dy in sides]
    pack(0)
    pack(1)
    for offsets in near:
        send_rows(*peer(*offsets))
    send_rows(a, bx * 2 + 1 - bc)

    @pl.when(bc == 1)
    def _():
        for offsets in far:
            send_rows(*peer(*offsets))

    recv[me] = send[me]
    wrecv[me] = wsend[me]


    plane[...] = dot(txr_ref[...], hot_rows(info[3:4, :], points)) * dot(
        tzr_ref[...], hot_rows(info[5:6, :], points)
    )
    second[...] = dot(tyr_ref[...], hot_rows(info[4:5, :], points))

    def forward(to_b):
        def one(jj, _):
            scaled = (plane[...] * second[pl.ds(to_b * modes_y + jj, 1), :]).astype(BF16)
            result = dot(scaled, message[...])
            part[to_b, jj] = result.reshape(2, naz, share, width).astype(BF16)
            return 0

        lax.fori_loop(0, modes_y, one, 0)

    def core_copy(to_x):
        return remote(
            part.at[to_x * 2 + (1 - bc)], from_core.at[to_x], core_s.at[to_x], core_r.at[to_x], a, bx * 2 + (1 - bc)
        )

    def quad_copy(kx, ky):
        to_x, to_y = (bx + kx) % nbx, (ay + ky) % 2
        k = kx * 2 + ky
        return remote(
            part.at[to_x * 2 + bc, :, to_y], from_quad.at[k], quad_s.at[k], quad_r.at[k],
            az * 2 + to_y, to_x * 2 + bc,
        )

    def line_copy(k, inward=False):
        to_z = (az + turn * k + naz) % naz
        at_z = to_z if inward else az
        return remote(quad.at[:, to_z], from_line.at[at_z], line_s.at[to_z], line_r.at[at_z], to_z * 2 + ay, b)

    for kx in range(nbx):
        to_x = (bx + 1 + kx) % nbx
        forward(to_x * 2 + (1 - bc))
        core_copy(to_x).start()
    for kx in range(nbx):
        to_x = (bx + 1 + kx) % nbx
        forward(to_x * 2 + bc)
        core_copy(to_x).wait_recv()
        part[to_x * 2 + bc] = (part[to_x * 2 + bc].astype(F32) + from_core[to_x].astype(F32)).astype(BF16)
        for ky in (1, 0):
            k = (1 + kx) % nbx
            if (k, ky) != (0, 0):
                quad_copy(k, ky).start()


    def position(i, _):
        here = pl.ds(pl.multiple_of(i * block, block), block)
        plane_c[here, :] = (
            dot(hot_columns(cols[here, 3:4], block), txc_ref[...])
            * dot(hot_columns(cols[here, 5:6], block), tzc_ref[...])
        ).astype(BF16)
        hot_y = hot_columns(cols[here, 4:5], block)
        for j in range(modes):
            second_c[j, here, :] = dot(hot_y, tyc_ref[j]).astype(BF16)
        return 0

    lax.fori_loop(0, points // block, position, 0)

    @pl.when(bc == 0)
    def _():
        for offsets in far[: len(far) // 3]:
            send_rows(*peer(*offsets))


    sums = part[b, :, ay].astype(F32)
    for kx in range(nbx):
        for ky in range(2):
            if (kx, ky) != (0, 0):
                quad_copy(kx, ky).wait_recv()
                sums = sums + from_quad[kx * 2 + ky].astype(F32)
    quad[...] = sums.astype(BF16)

    for k in FAR(naz):
        line_copy(k).start()

    @pl.when(bc == 0)
    def _():
        for offsets in far[len(far) // 3 :]:
            send_rows(*peer(*offsets))

    def gline_copy(k, inward=False):
        to_z = (az + turn * k + naz) % naz
        at_z = to_z if inward else az
        here = whole.at[b, :, ay, at_z]
        return remote(here, here, gline_s.at[to_z], gline_r.at[at_z], to_z * 2 + ay, b)

    def gquad_copy(kx, ky, at_x, at_y):
        to_x, to_y = (bx + kx) % nbx, (ay + ky) % 2
        k = kx * 2 + ky
        here = whole.at[at_x * 2 + bc, :, at_y]
        return remote(here, here, gquad_s.at[k], gquad_r.at[k], az * 2 + to_y, to_x * 2 + bc)

    def gcore_copy(k, at_x, at_y, at_c):
        here = whole.at[at_x * 2 + at_c, :, at_y]
        return remote(here, here, gcore_s.at[k], gcore_r.at[k], a, bx * 2 + (1 - bc))


    spec_copy.wait()
    sums = quad[:, az].astype(F32)
    for k in range(1, naz):
        line_copy(k, True).wait_recv()
        sums = sums + from_line[(az + turn * k + naz) % naz].astype(F32)
    mixed[...] = sums.reshape(modes_y * share, width)


    row_at = lax.broadcasted_iota(jnp.int32, (8, width), 0)

    def mix_step(i, _):
        rows = mixed[pl.ds(pl.multiple_of(i * 8, 8), 8), :].astype(BF16)
        out = jnp.zeros((8, width), F32)
        for r in range(8):
            out = jnp.where(row_at == r, dot(rows, spec[i * 8 + r]), out)
        mixed[pl.ds(pl.multiple_of(i * 8, 8), 8), :] = out
        return 0

    lax.fori_loop(0, modes_y * share // 8, mix_step, 0)
    whole[b, :, ay, az] = mixed[...].reshape(modes_y, share, width).astype(BF16)

    for k in FAR(naz):
        gline_copy(k).start()


    def arrived(i, _):
        src = (me + i) % n
        remote(wsend.at[src], wrecv.at[src], where_s.at[src], where_r.at[src], src // nb, src % nb).wait_recv()
        remote(send.at[src], recv.at[src], rows_s.at[src], rows_r.at[src], src // nb, src % nb).wait_recv()
        return 0

    lax.fori_loop(1, n, arrived, 0)

    for tile in range(n):
        wrow[:, tile * cap : (tile + 1) * cap] = wrecv[tile][:, :cap]
    diagonal = lax.broadcasted_iota(jnp.int32, (cap, LANES), 0) == lax.broadcasted_iota(jnp.int32, (cap, LANES), 1)

    def back_rows(to_a, to_b):
        row_copy(back, ret, ret_s, ret_r, to_a, to_b).start()

    def merge(dy, zero, count):
        def one(i, _):
            dz = (zero + i) % naz
            to_a = (az + turn * dz + naz) % naz * 2 + (ay + dy) % 2
            column = jnp.concatenate(
                [
                    jnp.sum(jnp.where(diagonal, wrecv[to_a * nb + to_b], 0.0), axis=1, keepdims=True)
                    for to_b in range(nb)
                ],
                axis=0,
            )
            same = (column == wrow[...]).astype(F32).astype(BF16)
            rows = dot(same, rows_of(recv[...], n * cap, width))
            for to_b in range(nb):
                back[to_a * nb + to_b] = rows[to_b * cap : (to_b + 1) * cap].astype(BF16)
            if dy == 0:
                for dc in range(2):
                    to_b = bx * 2 + (bc + dc) % 2

                    @pl.when(to_a * nb + to_b != me)
                    def _():
                        back_rows(to_a, to_b)

            return 0

        lax.fori_loop(0, count, one, 0)

    def far_back(first, last):
        for offsets in far[first:last]:
            back_rows(*peer(*offsets))

    merge(0, naz // 2, 1)
    merge(0, 0, 1)
    merge(1, 0, 1)
    for offsets in near:
        back_rows(*peer(*offsets))
    ret[me] = back[me]
    slab = 2 * nb

    def unpack(dz, first):

        at_z = (az + turn * dz + naz) % naz
        for q in range(slab):
            src = at_z * slab + q

            @pl.when(src != me)
            def _():
                remote(back.at[src], ret.at[src], ret_s.at[src], ret_r.at[src], src // nb, src % nb).wait_recv()


        rows = rows_of(ret[pl.ds(at_z * slab, slab)], slab * cap, width)
        base = (at_z * slab * cap).astype(F32)

        def one(i, _):
            here = pl.ds(pl.multiple_of(i * block, block), block)
            lane = lax.broadcasted_iota(jnp.int32, (block, slab * cap), 1).astype(F32) + base
            hot = (lane == cols[here, 0:1]).astype(F32).astype(BF16)
            value = dot(hot, rows)
            latent[here, :] = value if first else latent[here, :] + value
            return 0

        lax.fori_loop(0, points // block, one, 0)


    for k in range(1, naz):
        gline_copy(k, True).wait_recv()
    for kx in range(nbx):
        for ky in range(2):
            if (kx, ky) != (0, 0):
                gquad_copy(kx, ky, bx, ay).start()


    merge(0, naz // 2 + 1, naz - naz // 2 - 1)
    merge(0, 1, naz // 2 - 1)
    merge(1, 1, naz - 1)

    half = pairs // 2

    def inverse(at_b, at_y, first):
        part_b = rows_of(whole[at_b, :, at_y].reshape(modes_y, naz * share, width), modes_y * half, width)

        def one(i, _):
            here = pl.ds(pl.multiple_of(i * block, block), block)
            base = plane_c[here, pl.ds(pl.multiple_of(at_y * half, half), half)]
            scaled = [base * second_c[at_b * modes_y + jj, here, :] for jj in range(modes_y)]
            value = dot(jnp.concatenate(scaled, axis=1), part_b)
            total[here, :] = value if first else total[here, :] + value
            return 0

        lax.fori_loop(0, points // block, one, 0)

    def take(kx, ky):
        at_x, at_y = (bx + nbx - kx) % nbx, (ay + ky) % 2
        first = (kx, ky) == (0, 0)
        if not first:

            gquad_copy(kx, ky, at_x, at_y).wait_recv()

        gcore_copy(kx * 2 + ky, at_x, at_y, bc).start()
        inverse(at_x * 2 + bc, at_y, first)
        if first:
            far_back(0, len(far) // 3)

        gcore_copy(kx * 2 + ky, at_x, at_y, 1 - bc).wait_recv()

        inverse(at_x * 2 + (1 - bc), at_y, False)
        if first:
            far_back(len(far) // 3, len(far))

    take(0, 0)
    unpack(0, True)
    quarters = [(kx, ky) for kx in range(nbx) for ky in range(2)][1:]
    for kx, ky in quarters:
        take(kx, ky)
    for dz in FAR(naz):
        unpack(dz, False)

    def left(i, _):
        src = (me + i) % n
        row_copy(back, ret, ret_s, ret_r, src // nb, src % nb).wait_send()
        row_copy(wsend, wrecv, where_s, where_r, src // nb, src % nb).wait_send()
        row_copy(send, recv, rows_s, rows_r, src // nb, src % nb).wait_send()
        return 0

    lax.fori_loop(1, n, left, 0)


    def decode(i, _):
        here = pl.ds(pl.multiple_of(i * block, block), block)
        latent_out = jax.nn.gelu(total[here, :] + dot(latent[here, :].astype(BF16), ws_ref[...])).astype(BF16)
        gathered = (cols[here, 7:8] * latent_out.astype(F32)).astype(BF16)
        out_ref[here, :] = jax.nn.gelu(dot(gathered, wh_ref[...])).astype(BF16)
        return 0

    lax.fori_loop(0, points // block, decode, 0)


    for to_x in range(nbx):
        core_copy(to_x).wait_send()
    for kx in range(nbx):
        for ky in range(2):
            gcore_copy(kx * 2 + ky, bx, ay, bc).wait_send()
            if (kx, ky) != (0, 0):
                quad_copy(kx, ky).wait_send()
                gquad_copy(kx, ky, bx, ay).wait_send()
    for k in range(1, naz):
        line_copy(k).wait_send()
        gline_copy(k).wait_send()


def per_device(
    features,
    tile_ids,
    cell_ids,
    spread_weight,
    read_weight,
    message_weight,
    skip_weight,
    spectral_weight,
    hidden_weight,
    output_weight,
):
    points, width = features.shape
    na = lax.axis_size("aa")
    nb = lax.axis_size("ba")
    n = na * nb
    cap = 3 * points // (2 * n)
    modes_y, share = spectral_weight.shape[0], spectral_weight.shape[1]
    modes = modes_y * nb
    pairs = share * na
    naz, nbx = na // 2, nb // 2

    order = np.arange(pairs).reshape(naz, 2, share).transpose(1, 0, 2).reshape(pairs)
    basis = basis_np(modes, G)
    tx = split_table(np.repeat(basis, modes, axis=0)[order].T)
    tz = split_table(np.tile(basis, (modes, 1))[order].T)
    ty = split_table(basis.T)
    tables = [jnp.asarray(np.ascontiguousarray(t.T)) for t in (tx, ty, tz)] + [
        jnp.asarray(t) for t in (tx, np.repeat(ty.T[:, :, None], pairs // 2, axis=2), tz)
    ]

    spec = spectral_weight.reshape(modes_y * share, width, width)

    inputs = [
        tile_ids.reshape(1, points), cell_ids.reshape(1, points), spread_weight.reshape(1, points),
        read_weight.reshape(1, points), features, message_weight, skip_weight, hidden_weight, *tables,
    ]
    vmem = pl.BlockSpec(memory_space=pltpu.VMEM)
    dma = pltpu.SemaphoreType.DMA
    hidden = pl.pallas_call(
        functools.partial(layer_kernel, (na, nb, cap, modes_y, share)),
        in_specs=[pl.BlockSpec(memory_space=pl.ANY)] * (len(inputs) + 1),
        out_specs=vmem,
        out_shape=pltpu.VMEM((points, width), BF16),
        scratch_shapes=[
            pltpu.VMEM((modes_y * share, width, width), BF16),
            pltpu.VMEM((8, points), F32),
            pltpu.VMEM((1, points), F32),
            pltpu.VMEM((points, 8), F32),
            pltpu.VMEM((points, width), BF16),
            pltpu.VMEM((pairs, points), F32),
            pltpu.VMEM((modes, points), F32),
            pltpu.VMEM((points, pairs), BF16),
            pltpu.VMEM((modes, points, pairs // 2), BF16),
            pltpu.VMEM((points, width), F32),
            pltpu.VMEM((points, width), F32),
            pltpu.VMEM((n, cap, width), BF16),
            pltpu.VMEM((n, cap, width), BF16),
            pltpu.VMEM((n, cap, width), BF16),
            pltpu.VMEM((n, cap, width), BF16),
            pltpu.VMEM((n, 1, LANES), F32),
            pltpu.VMEM((n, 1, LANES), F32),
            pltpu.VMEM((1, n * cap), F32),
            pltpu.VMEM((nb, modes_y, 2, naz, share, width), BF16),
            pltpu.VMEM((nbx, modes_y, 2, naz, share, width), BF16),
            pltpu.VMEM((2 * nbx, modes_y, naz, share, width), BF16),
            pltpu.VMEM((modes_y, naz, share, width), BF16),
            pltpu.VMEM((naz, modes_y, share, width), BF16),
            pltpu.VMEM((modes_y * share, width), F32),
            pltpu.VMEM((nb, modes_y, 2, naz, share, width), BF16),
            dma, dma((n,)), dma((n,)), dma((n,)), dma((n,)), dma((n,)), dma((n,)),
            dma((nbx,)), dma((nbx,)), dma((2 * nbx,)), dma((2 * nbx,)), dma((naz,)), dma((naz,)),
            dma((naz,)), dma((naz,)), dma((2 * nbx,)), dma((2 * nbx,)), dma((2 * nbx,)), dma((2 * nbx,)),
            dma((len(inputs),)),
        ] + [pltpu.VMEM(value.shape, value.dtype) for value in inputs],
        compiler_params=pltpu.CompilerParams(
            collective_id=0, has_side_effects=True, vmem_limit_bytes=56 * 1024 * 1024
        ),
        name="layer",
    )(*inputs, spec)
    return dot(hidden, output_weight).astype(BF16)


def solution(mesh):
    placed = (
        P(("aa", "ba"), None),
        P(("aa", "ba"), None),
        P(("aa", "ba")),
        P(("aa", "ba")),
        P(("aa", "ba")),
        P(),
        P(),
        P("ba", "aa", None, None),
        P(),
        P(),
    )
    return jax.shard_map(
        per_device, mesh=mesh, in_specs=placed, out_specs=P(("aa", "ba"), None), check_vma=False
    )
```

```python
import functools
import math

import jax
import jax.numpy as jnp
import numpy as np
from jax import lax
from jax.experimental import pallas as pl
from jax.experimental.pallas import tpu as pltpu
from jax.sharding import PartitionSpec as P

G = 64
LANES = 128
F32 = jnp.float32
BF16 = jnp.bfloat16
PACE = (4, 4, 0, 0, 18)
MESH = pl.DeviceIdType.MESH


def FAR(size):
    return [(size // 2 + i) % size for i in range(size) if (size // 2 + i) % size]


def basis_np(modes, grid):
    k = np.arange(modes)[:, None]
    half = modes // 2
    freq = np.where(k < half, k, k - half + 1).astype(np.float64)
    phase = 2.0 * math.pi * freq * np.arange(grid)[None, :] / grid
    wave = np.where(k < half, np.cos(phase), np.sin(phase))
    norm = np.where(k == 0, math.sqrt(1.0 / grid), math.sqrt(2.0 / grid))
    return (wave * norm).astype(np.float32)


def split_table(table):
    high = table.astype(BF16)
    low = (table - high.astype(np.float32)).astype(BF16)
    return np.concatenate([high, low], axis=0)


def dot(a, b):
    return jnp.dot(a, b, preferred_element_type=F32)


def rows_of(block, *shape):
    if any(size % 16 for size in (block.shape[-2], shape[-2])):
        return block.astype(F32).reshape(shape).astype(BF16)
    return block.reshape(shape)


def hot_rows(values, points):
    lane = lax.broadcasted_iota(jnp.int32, (2 * G, points), 0) % G
    return (lane.astype(F32) == values).astype(F32).astype(BF16)


def hot_columns(values, points):
    lane = lax.broadcasted_iota(jnp.int32, (points, 2 * G), 1) % G
    return (lane.astype(F32) == values).astype(F32).astype(BF16)


def layer_kernel(
    sizes,
    tile_hbm, cell_hbm, spread_hbm, read_hbm, feat_hbm, wm_hbm, ws_hbm, wh_hbm, txr_hbm, tyr_hbm, tzr_hbm, txc_hbm, tyc_hbm, tzc_hbm,
    spec_hbm, out_ref,
    spec, info, slots, cols, message, plane, second, plane_c, second_c, total, latent,
    send, recv, back, ret, wsend, wrecv, wrow,
    part, from_core, from_quad, quad, from_line, mixed, whole,
    spec_sem, where_s, where_r, rows_s, rows_r, ret_s, ret_r,
    core_s, core_r, quad_s, quad_r, line_s, line_r,
    gline_s, gline_r, gquad_s, gquad_r, gcore_s, gcore_r, load_sem,
    tile_ref, cell_ref, spread_ref, read_ref, feat_ref, wm_ref, ws_ref, wh_ref, txr_ref, tyr_ref, tzr_ref, txc_ref, tyc_ref, tzc_ref,
):
    na, nb, cap, modes_y, share = sizes
    n = na * nb
    naz, nbx = na // 2, nb // 2
    points, width = feat_ref.shape
    pairs = txr_ref.shape[0]
    modes = modes_y * nb
    a = lax.axis_index("aa")
    b = lax.axis_index("ba")
    me = a * nb + b
    az, ay, bx, bc = a // 2, a % 2, b // 2, b % 2
    turn = 1 - 2 * (az // (naz // 2))

    def remote(src, dst, send_sem, recv_sem, to_a, to_b):
        return pltpu.make_async_remote_copy(
            src_ref=src, dst_ref=dst, send_sem=send_sem, recv_sem=recv_sem,
            device_id={"aa": to_a, "ba": to_b}, device_id_type=MESH,
        )


    loads = [
        pltpu.make_async_copy(src, dst, load_sem.at[i])
        for i, (src, dst) in enumerate([
            (tile_hbm, tile_ref), (cell_hbm, cell_ref), (spread_hbm, spread_ref), (read_hbm, read_ref),
            (feat_hbm, feat_ref), (wm_hbm, wm_ref), (ws_hbm, ws_ref), (wh_hbm, wh_ref), (txr_hbm, txr_ref),
            (tyr_hbm, tyr_ref), (tzr_hbm, tzr_ref), (txc_hbm, txc_ref), (tyc_hbm, tyc_ref), (tzc_hbm, tzc_ref),
        ])
    ]
    barrier = pltpu.get_barrier_semaphore()

    def greet(k, _):
        peer = (me + k) % n
        pl.semaphore_signal(
            barrier, inc=1, device_id={"aa": peer // nb, "ba": peer % nb}, device_id_type=MESH
        )
        return 0

    lax.fori_loop(1, n, greet, 0)
    for load in loads:
        load.start()
    spec_copy = pltpu.make_async_copy(spec_hbm, spec, spec_sem)
    spec_copy.start()


    for load in loads[:4]:
        load.wait()
    tile = tile_ref[...].astype(F32)
    cell = cell_ref[...].astype(F32)
    tile_x, tile_y = G // na, G // nb
    row = jnp.floor((tile + 0.5) * (1.0 / nb))
    high = jnp.floor((cell + 0.5) * (1.0 / G))
    deep = jnp.floor((high + 0.5) * (1.0 / tile_y))
    low = cell - high * G
    info[0:1, :] = tile
    info[1:2, :] = high
    info[2:3, :] = low
    info[3:4, :] = row * tile_x + deep
    info[4:5, :] = (tile - row * nb) * tile_y + (high - deep * tile_y)
    info[5:6, :] = low
    info[6:7, :] = spread_ref[...]
    info[7:8, :] = read_ref[...]

    step = 256
    upper = (
        lax.broadcasted_iota(jnp.int32, (step, step), 0) <= lax.broadcasted_iota(jnp.int32, (step, step), 1)
    ).astype(F32).astype(BF16)
    carry = jnp.zeros((n, 1), F32)
    tile_at = lax.broadcasted_iota(jnp.int32, (n, step), 0).astype(F32)
    rank_at = lax.broadcasted_iota(jnp.int32, (LANES, step), 0).astype(F32)
    found = jnp.zeros((3 * n, LANES), F32)
    for start in range(0, points, step):
        piece = slice(start, start + step)
        tiles = info[0:1, piece]
        hot = (tile_at == tiles).astype(F32)
        counts = dot(hot.astype(BF16), upper) + carry
        rank = jnp.sum(counts * hot, axis=0, keepdims=True) - 1.0
        slots[:, piece] = tiles * cap + rank
        carry = carry + jnp.sum(hot, axis=1, keepdims=True)
        marks = jnp.concatenate([hot * info[1:2, piece], hot * info[2:3, piece], hot], axis=0).astype(BF16)
        ranks = (rank_at == rank).astype(F32).astype(BF16)
        found = found + lax.dot_general(marks, ranks, (((1,), (1,)), ((), ())), preferred_element_type=F32)
    where = found[:n] * G + found[n : 2 * n] + (found[2 * n :] - 1.0)
    for tile in range(n):
        wsend[tile] = where[tile : tile + 1, :]
    for start in range(0, points, LANES):
        piece = slice(start, start + LANES)
        both = jnp.concatenate([slots[:, piece], info[1:8, piece]], axis=0)
        cols[piece, :] = both.T

    for load in loads[4:]:
        load.wait()
    message[...] = (cols[:, 6:7] * dot(feat_ref[...], wm_ref[...])).astype(BF16)


    pl.semaphore_wait(barrier, n - 1)


    block = 1024

    group = nb * cap
    own = lax.broadcasted_iota(jnp.int32, (group, points), 0).astype(F32)

    def row_copy(src, dst, sem_s, sem_r, to_a, to_b):
        return remote(src.at[to_a * nb + to_b], dst.at[me], sem_s.at[to_a * nb + to_b], sem_r.at[me], to_a, to_b)

    def peer(dz, dy, dx, dc):
        return (az + turn * dz + naz) % naz * 2 + (ay + dy) % 2, (bx + dx) % nbx * 2 + (bc + dc) % 2

    def send_rows(to_a, to_b):
        row_copy(wsend, wrecv, where_s, where_r, to_a, to_b).start()
        row_copy(send, recv, rows_s, rows_r, to_a, to_b).start()

    def pack(dy):
        def one(i, _):
            dz = (naz // 2 + i) % naz
            to_a = (az + turn * dz + naz) % naz * 2 + (ay + dy) % 2
            base = (to_a * group).astype(F32)
            hot = (own == slots[...] - base).astype(F32).astype(BF16)
            rows = dot(hot, message[...])
            for to_b in range(nb):
                send[to_a * nb + to_b] = rows[to_b * cap : (to_b + 1) * cap].astype(BF16)
            if dy == 0:

                @pl.when(to_a != a)
                def _():
                    for dc in range(2):
                        send_rows(to_a, bx * 2 + (bc + dc) % 2)

            return 0

        lax.fori_loop(0, naz, one, 0)

    sides = [(dx, dy) for dx in range(nbx) for dy in range(2) if (dx, dy) != (0, 0)]
    far = [(dz, dy, dx, dc) for dz in FAR(naz) for dc in range(2) for dx, dy in sides]
    near = [(0, dy, dx, dc) for dc in range(2) for dx, dy in sides]
    pack(0)
    pack(1)
    for offsets in near:
        send_rows(*peer(*offsets))
    send_rows(a, bx * 2 + 1 - bc)

    @pl.when(bc == 1)
    def _():
        for offsets in far:
            send_rows(*peer(*offsets))

    recv[me] = send[me]
    wrecv[me] = wsend[me]


    plane[...] = dot(txr_ref[...], hot_rows(info[3:4, :], points)) * dot(
        tzr_ref[...], hot_rows(info[5:6, :], points)
    )
    second[...] = dot(tyr_ref[...], hot_rows(info[4:5, :], points))

    def forward(to_b):
        def one(jj, _):
            scaled = (plane[...] * second[pl.ds(to_b * modes_y + jj, 1), :]).astype(BF16)
            result = dot(scaled, message[...])
            part[to_b, jj] = result.reshape(2, naz, share, width).astype(BF16)
            return 0

        lax.fori_loop(0, modes_y, one, 0)

    def core_copy(to_x):
        return remote(
            part.at[to_x * 2 + (1 - bc)], from_core.at[to_x], core_s.at[to_x], core_r.at[to_x], a, bx * 2 + (1 - bc)
        )

    def quad_copy(kx, ky):
        to_x, to_y = (bx + kx) % nbx, (ay + ky) % 2
        k = kx * 2 + ky
        return remote(
            part.at[to_x * 2 + bc, :, to_y], from_quad.at[k], quad_s.at[k], quad_r.at[k],
            az * 2 + to_y, to_x * 2 + bc,
        )

    def line_copy(k, inward=False):
        to_z = (az + turn * k + naz) % naz
        at_z = to_z if inward else az
        return remote(quad.at[:, to_z], from_line.at[at_z], line_s.at[to_z], line_r.at[at_z], to_z * 2 + ay, b)

    for kx in range(nbx):
        to_x = (bx + 1 + kx) % nbx
        forward(to_x * 2 + (1 - bc))
        core_copy(to_x).start()
    for kx in range(nbx):
        to_x = (bx + 1 + kx) % nbx
        forward(to_x * 2 + bc)
        core_copy(to_x).wait_recv()
        part[to_x * 2 + bc] = (part[to_x * 2 + bc].astype(F32) + from_core[to_x].astype(F32)).astype(BF16)
        for ky in (1, 0):
            k = (1 + kx) % nbx
            if (k, ky) != (0, 0):
                quad_copy(k, ky).start()


    def position(i, _):
        here = pl.ds(pl.multiple_of(i * block, block), block)
        plane_c[here, :] = (
            dot(hot_columns(cols[here, 3:4], block), txc_ref[...])
            * dot(hot_columns(cols[here, 5:6], block), tzc_ref[...])
        ).astype(BF16)
        hot_y = hot_columns(cols[here, 4:5], block)
        for j in range(modes):
            second_c[j, here, :] = dot(hot_y, tyc_ref[j]).astype(BF16)
        return 0

    lax.fori_loop(0, points // block, position, 0)

    @pl.when(bc == 0)
    def _():
        for offsets in far[: len(far) * 8 // 18]:
            send_rows(*peer(*offsets))


    sums = part[b, :, ay].astype(F32)
    for kx in range(nbx):
        for ky in range(2):
            if (kx, ky) != (0, 0):
                quad_copy(kx, ky).wait_recv()
                sums = sums + from_quad[kx * 2 + ky].astype(F32)
    quad[...] = sums.astype(BF16)

    for k in FAR(naz):
        line_copy(k).start()

    @pl.when(bc == 0)
    def _():
        for offsets in far[len(far) * 8 // 18 :]:
            send_rows(*peer(*offsets))

    def gline_copy(k, inward=False):
        to_z = (az + turn * k + naz) % naz
        at_z = to_z if inward else az
        here = whole.at[b, :, ay, at_z]
        return remote(here, here, gline_s.at[to_z], gline_r.at[at_z], to_z * 2 + ay, b)

    def gquad_copy(kx, ky, at_x, at_y):
        to_x, to_y = (bx + kx) % nbx, (ay + ky) % 2
        k = kx * 2 + ky
        here = whole.at[at_x * 2 + bc, :, at_y]
        return remote(here, here, gquad_s.at[k], gquad_r.at[k], az * 2 + to_y, to_x * 2 + bc)

    def gcore_copy(k, at_x, at_y, at_c):
        here = whole.at[at_x * 2 + at_c, :, at_y]
        return remote(here, here, gcore_s.at[k], gcore_r.at[k], a, bx * 2 + (1 - bc))


    spec_copy.wait()
    sums = quad[:, az].astype(F32)
    for k in range(1, naz):
        line_copy(k, True).wait_recv()
        sums = sums + from_line[(az + turn * k + naz) % naz].astype(F32)
    mixed[...] = sums.reshape(modes_y * share, width)


    row_at = lax.broadcasted_iota(jnp.int32, (8, width), 0)

    def mix_step(i, _):
        rows = mixed[pl.ds(pl.multiple_of(i * 8, 8), 8), :].astype(BF16)
        out = jnp.zeros((8, width), F32)
        for r in range(8):
            out = jnp.where(row_at == r, dot(rows, spec[i * 8 + r]), out)
        mixed[pl.ds(pl.multiple_of(i * 8, 8), 8), :] = out
        return 0

    lax.fori_loop(0, modes_y * share // 8, mix_step, 0)
    whole[b, :, ay, az] = mixed[...].reshape(modes_y, share, width).astype(BF16)

    for k in FAR(naz):
        gline_copy(k).start()


    def arrived(i, _):
        src = (me + i) % n
        remote(wsend.at[src], wrecv.at[src], where_s.at[src], where_r.at[src], src // nb, src % nb).wait_recv()
        remote(send.at[src], recv.at[src], rows_s.at[src], rows_r.at[src], src // nb, src % nb).wait_recv()
        return 0

    lax.fori_loop(1, n, arrived, 0)

    for tile in range(n):
        wrow[:, tile * cap : (tile + 1) * cap] = wrecv[tile][:, :cap]
    diagonal = lax.broadcasted_iota(jnp.int32, (cap, LANES), 0) == lax.broadcasted_iota(jnp.int32, (cap, LANES), 1)

    def back_rows(to_a, to_b):
        row_copy(back, ret, ret_s, ret_r, to_a, to_b).start()

    def merge(dy, zero, count):
        def one(i, _):
            dz = (zero + i) % naz
            to_a = (az + turn * dz + naz) % naz * 2 + (ay + dy) % 2
            column = jnp.concatenate(
                [
                    jnp.sum(jnp.where(diagonal, wrecv[to_a * nb + to_b], 0.0), axis=1, keepdims=True)
                    for to_b in range(nb)
                ],
                axis=0,
            )
            same = (column == wrow[...]).astype(F32).astype(BF16)
            rows = dot(same, rows_of(recv[...], n * cap, width))
            for to_b in range(nb):
                back[to_a * nb + to_b] = rows[to_b * cap : (to_b + 1) * cap].astype(BF16)
            if dy == 0:
                for dc in range(2):
                    to_b = bx * 2 + (bc + dc) % 2

                    @pl.when(to_a * nb + to_b != me)
                    def _():
                        back_rows(to_a, to_b)

            return 0

        lax.fori_loop(0, count, one, 0)

    def far_back(first, last):
        for offsets in far[first:last]:
            back_rows(*peer(*offsets))

    merge(0, naz // 2, 1)
    merge(0, 0, 1)
    merge(1, 0, 1)
    for offsets in near:
        back_rows(*peer(*offsets))
    ret[me] = back[me]
    slab = 2 * nb

    def unpack(dz, first, last=False):

        at_z = (az + turn * dz + naz) % naz
        for q in range(slab):
            src = at_z * slab + q

            @pl.when(src != me)
            def _():
                remote(back.at[src], ret.at[src], ret_s.at[src], ret_r.at[src], src // nb, src % nb).wait_recv()


        rows = rows_of(ret[pl.ds(at_z * slab, slab)], slab * cap, width)
        base = (at_z * slab * cap).astype(F32)

        def one(i, _):
            here = pl.ds(pl.multiple_of(i * block, block), block)
            lane = lax.broadcasted_iota(jnp.int32, (block, slab * cap), 1).astype(F32) + base
            hot = (lane == cols[here, 0:1]).astype(F32).astype(BF16)
            value = dot(hot, rows)
            value = value if first else latent[here, :] + value
            if not last:
                latent[here, :] = value
                return 0
            latent_out = jax.nn.gelu(total[here, :] + dot(value.astype(BF16), ws_ref[...])).astype(BF16)
            gathered = (cols[here, 7:8] * latent_out.astype(F32)).astype(BF16)
            out_ref[here, :] = jax.nn.gelu(dot(gathered, wh_ref[...])).astype(BF16)
            return 0

        lax.fori_loop(0, points // block, one, 0)


    for k in range(1, naz):
        gline_copy(k, True).wait_recv()
    for kx in range(nbx):
        for ky in range(2):
            if (kx, ky) != (0, 0):
                gquad_copy(kx, ky, bx, ay).start()


    merge(0, naz // 2 + 1, naz - naz // 2 - 1)
    merge(0, 1, naz // 2 - 1)
    merge(1, 1, naz - 1)

    half = pairs // 2

    def inverse(at_b, at_y, first):
        part_b = rows_of(whole[at_b, :, at_y].reshape(modes_y, naz * share, width), modes_y * half, width)

        def one(i, _):
            here = pl.ds(pl.multiple_of(i * block, block), block)
            base = plane_c[here, pl.ds(pl.multiple_of(at_y * half, half), half)]
            scaled = [base * second_c[at_b * modes_y + jj, here, :] for jj in range(modes_y)]
            value = dot(jnp.concatenate(scaled, axis=1), part_b)
            total[here, :] = value if first else total[here, :] + value
            return 0

        lax.fori_loop(0, points // block, one, 0)

    def take(kx, ky):
        at_x, at_y = (bx + nbx - kx) % nbx, (ay + ky) % 2
        first = (kx, ky) == (0, 0)
        if not first:

            gquad_copy(kx, ky, at_x, at_y).wait_recv()

        gcore_copy(kx * 2 + ky, at_x, at_y, bc).start()
        inverse(at_x * 2 + bc, at_y, first)
        if first:
            far_back(0, len(far) // 3)

        gcore_copy(kx * 2 + ky, at_x, at_y, 1 - bc).wait_recv()

        inverse(at_x * 2 + (1 - bc), at_y, False)
        if first:
            far_back(len(far) // 3, len(far))

    take(0, 0)
    unpack(0, True)
    quarters = [(kx, ky) for kx in range(nbx) for ky in range(2)][1:]
    for kx, ky in quarters:
        take(kx, ky)
    for dz in FAR(naz):
        unpack(dz, False, dz == FAR(naz)[-1])

    def left(i, _):
        src = (me + i) % n
        row_copy(back, ret, ret_s, ret_r, src // nb, src % nb).wait_send()
        row_copy(wsend, wrecv, where_s, where_r, src // nb, src % nb).wait_send()
        row_copy(send, recv, rows_s, rows_r, src // nb, src % nb).wait_send()
        return 0

    lax.fori_loop(1, n, left, 0)


    for to_x in range(nbx):
        core_copy(to_x).wait_send()
    for kx in range(nbx):
        for ky in range(2):
            gcore_copy(kx * 2 + ky, bx, ay, bc).wait_send()
            if (kx, ky) != (0, 0):
                quad_copy(kx, ky).wait_send()
                gquad_copy(kx, ky, bx, ay).wait_send()
    for k in range(1, naz):
        line_copy(k).wait_send()
        gline_copy(k).wait_send()


def per_device(
    features,
    tile_ids,
    cell_ids,
    spread_weight,
    read_weight,
    message_weight,
    skip_weight,
    spectral_weight,
    hidden_weight,
    output_weight,
):
    points, width = features.shape
    na = lax.axis_size("aa")
    nb = lax.axis_size("ba")
    n = na * nb
    cap = 3 * points // (2 * n)
    modes_y, share = spectral_weight.shape[0], spectral_weight.shape[1]
    modes = modes_y * nb
    pairs = share * na
    naz, nbx = na // 2, nb // 2

    order = np.arange(pairs).reshape(naz, 2, share).transpose(1, 0, 2).reshape(pairs)
    basis = basis_np(modes, G)
    tx = split_table(np.repeat(basis, modes, axis=0)[order].T)
    tz = split_table(np.tile(basis, (modes, 1))[order].T)
    ty = split_table(basis.T)
    tables = [jnp.asarray(np.ascontiguousarray(t.T)) for t in (tx, ty, tz)] + [
        jnp.asarray(t) for t in (tx, np.repeat(ty.T[:, :, None], pairs // 2, axis=2), tz)
    ]

    spec = spectral_weight.reshape(modes_y * share, width, width)

    inputs = [
        tile_ids.reshape(1, points), cell_ids.reshape(1, points), spread_weight.reshape(1, points),
        read_weight.reshape(1, points), features, message_weight, skip_weight, hidden_weight, *tables,
    ]
    vmem = pl.BlockSpec(memory_space=pltpu.VMEM)
    dma = pltpu.SemaphoreType.DMA
    hidden = pl.pallas_call(
        functools.partial(layer_kernel, (na, nb, cap, modes_y, share)),
        in_specs=[pl.BlockSpec(memory_space=pl.ANY)] * (len(inputs) + 1),
        out_specs=vmem,
        out_shape=pltpu.VMEM((points, width), BF16),
        scratch_shapes=[
            pltpu.VMEM((modes_y * share, width, width), BF16),
            pltpu.VMEM((8, points), F32),
            pltpu.VMEM((1, points), F32),
            pltpu.VMEM((points, 8), F32),
            pltpu.VMEM((points, width), BF16),
            pltpu.VMEM((pairs, points), F32),
            pltpu.VMEM((modes, points), F32),
            pltpu.VMEM((points, pairs), BF16),
            pltpu.VMEM((modes, points, pairs // 2), BF16),
            pltpu.VMEM((points, width), F32),
            pltpu.VMEM((points, width), F32),
            pltpu.VMEM((n, cap, width), BF16),
            pltpu.VMEM((n, cap, width), BF16),
            pltpu.VMEM((n, cap, width), BF16),
            pltpu.VMEM((n, cap, width), BF16),
            pltpu.VMEM((n, 1, LANES), F32),
            pltpu.VMEM((n, 1, LANES), F32),
            pltpu.VMEM((1, n * cap), F32),
            pltpu.VMEM((nb, modes_y, 2, naz, share, width), BF16),
            pltpu.VMEM((nbx, modes_y, 2, naz, share, width), BF16),
            pltpu.VMEM((2 * nbx, modes_y, naz, share, width), BF16),
            pltpu.VMEM((modes_y, naz, share, width), BF16),
            pltpu.VMEM((naz, modes_y, share, width), BF16),
            pltpu.VMEM((modes_y * share, width), F32),
            pltpu.VMEM((nb, modes_y, 2, naz, share, width), BF16),
            dma, dma((n,)), dma((n,)), dma((n,)), dma((n,)), dma((n,)), dma((n,)),
            dma((nbx,)), dma((nbx,)), dma((2 * nbx,)), dma((2 * nbx,)), dma((naz,)), dma((naz,)),
            dma((naz,)), dma((naz,)), dma((2 * nbx,)), dma((2 * nbx,)), dma((2 * nbx,)), dma((2 * nbx,)),
            dma((len(inputs),)),
        ] + [pltpu.VMEM(value.shape, value.dtype) for value in inputs],
        compiler_params=pltpu.CompilerParams(
            collective_id=0, has_side_effects=True, vmem_limit_bytes=56 * 1024 * 1024
        ),
        name="layer",
    )(*inputs, spec)
    return dot(hidden, output_weight).astype(BF16)


def solution(mesh):
    placed = (
        P(("aa", "ba"), None),
        P(("aa", "ba"), None),
        P(("aa", "ba")),
        P(("aa", "ba")),
        P(("aa", "ba")),
        P(),
        P(),
        P("ba", "aa", None, None),
        P(),
        P(),
    )
    return jax.shard_map(
        per_device, mesh=mesh, in_specs=placed, out_specs=P(("aa", "ba"), None), check_vma=False
    )
```
